32 devices in a mesh: wide: 8 (over z, y), narrow: 4 (over x, core).
Axes of the slice: x: 2, y: 2, z: 4, core: 2. Of those that a mesh axis runs over, the one named last changes fastest.
Arguments:
- rhs: float32 [3, 32, 32, 128], P(None, 'wide', 'narrow'), may hold values from -12 to 12
- start: float32 [3, 32, 32, 128], P(None, 'wide', 'narrow'), may hold values from -2 to 2
- trans: float32 [3, 32, 32, 128], P(None, 'wide', 'narrow'), may hold values from 0.2 to 2
- accum: float32 [32, 32, 128], P('wide', 'narrow'), may hold values from 2 to 8
- coupling: float32 [3, 3, 32, 32, 128], P(None, None, 'wide', 'narrow'), may hold values from -0.3 to 0.3
- well_cells: int32 [8, 4, 64], P('wide', 'narrow'), may hold values from 0 to 4095
- well_index: float32 [8, 4, 64], P('wide', 'narrow'), may hold values from 1 to 20
- agg_map: int32 [32, 32, 128], P('wide', 'narrow'), may hold values from 0 to 31
- tile_factors: bfloat16 [48, 48, 128, 128], P('wide', 'narrow')
- coarse_inverse: float32 [1024, 1024], P(('wide', 'narrow')), as said below
Outputs:
- iterate: float32 [3, 32, 32, 128], P(None, 'wide', 'narrow')
- residual: float32 [3, 32, 32, 128], P(None, 'wide', 'narrow')
The draws below stay inside these ranges and needn't reach their ends.
Inputs may be any that keep to these rules, and one draw needn't show every extreme that they name: well_cells names, for each device's 64 connections, one of that device's own 4 * 8 * 128 cells, counted by pair, then column, then position in the tile; connections may share a cell. agg_map names one of the 32 aggregates of the device that owns the cell. coarse_inverse is symmetric.
All inputs are finite; a program needn't handle non-finite values.
Results may differ from the reference program's by a relative error of at most 0.00095.
Values sent between devices are 32-bit elements; how exact they have to be, the bound alone decides.
No kernel may reach another device: no remote copies, remote signals or barrier semaphores. Data moves between devices by JAX's collectives and lax.ppermute only.
A program may use at most 64 MiB of HBM per device.

```python
import math
import jax
import jax.numpy as jnp
from jax import lax

PHASES = 3
PX = 4
CY = 8
AGG_LOC = 32
CONN = 64
SWEEPS = 3
INNER = 3
TILE = 128
NX2 = 32
NY = 32
TX_ALL = 48
TY_ALL = 48
NAGG = 1024
N_WIDE = 8
N_NARROW = 4


def draw_tile_factors(key, part):
    full_shape = (TX_ALL, TY_ALL, TILE, TILE)
    deviation = 0.02 * jax.random.normal(key, full_shape, jnp.float32)
    return (jnp.eye(TILE, dtype=jnp.float32) + deviation).astype(jnp.bfloat16)


def draw_coarse_inverse(key, part):
    subkeys = jax.random.split(jax.random.fold_in(key, 7), 4)
    owners = NAGG // AGG_LOC
    shuffle = jax.random.permutation(subkeys[0], owners)
    position = jnp.argsort(shuffle)
    partner = shuffle[position ^ 1]
    device_of = jnp.arange(NAGG) // AGG_LOC
    paired = partner[device_of][:, None] == device_of[None, :]
    background = jax.random.normal(subkeys[1], (NAGG, NAGG), jnp.float32)
    partner_part = jax.random.normal(subkeys[2], (NAGG, NAGG), jnp.float32)
    diag_scale = jax.random.uniform(subkeys[3], (NAGG,), jnp.float32, 0.0005, 0.0015)
    back_scale = 5e-06
    sym_back = (background + background.T) * (back_scale / math.sqrt(2.0))
    sym_partner = (partner_part + partner_part.T) * (0.0004 / math.sqrt(2.0))
    return jnp.diag(diag_scale) + sym_back + jnp.where(paired, sym_partner, 0.0)


def set_ends(values, rng, smallest, high):
    longest = values.shape.index(max(values.shape))
    spots = []
    for shift in (0, 1):
        where = [jax.random.randint(jax.random.fold_in(rng, axis), (), 0, length) for axis, length in enumerate(values.shape)]
        where[longest] = (where[longest] + shift) % values.shape[longest]
        spots.append(tuple(where))
    return values.at[spots[0]].set(smallest).at[spots[1]].set(high)


def level_of(rng, shape, shards, least, largest):
    factor_of, own = 1.0, jax.random.fold_in(rng, 6)
    for dim, parts in shards:
        draws = jnp.exp(jax.random.uniform(jax.random.fold_in(own, dim), (parts,), jnp.float32, least / len(shards), largest / len(shards)))
        factor_of = factor_of * jnp.repeat(draws, shape[dim] // parts).reshape([-1 if axis == dim else 1 for axis in range(len(shape))])
    return factor_of


def normal_values(own_key, extent, width, limit, pieces=(), kind=jnp.bfloat16):
    entries = width * jax.random.normal(own_key, extent, jnp.float32)
    if pieces:
        entries = entries * level_of(own_key, extent, pieces, -0.22, 0.18)
    return jnp.clip(entries, -limit, limit).astype(kind)


def setup_inputs(seed: int = 0) -> dict:
    key_of = jax.random.split(jax.random.key(seed), 11)
    rhs = normal_values(key_of[0], (PHASES, NX2, NY, TILE), 2.0, 12.0, ((1, 8), (2, 4)), jnp.float32)
    start = normal_values(key_of[1], (PHASES, NX2, NY, TILE), 0.3, 2.0, ((1, 8), (2, 4)), jnp.float32)
    trans = jnp.clip(jnp.exp(math.log(2.0) - 2.3025851 * jax.random.uniform(key_of[2], (3, NX2, NY, TILE), jnp.float32) ** level_of(key_of[2], (3, NX2, NY, TILE), ((1, 8), (2, 4)), -0.2, 0.2)), 0.2, 2.0)
    accum = jnp.clip(jnp.exp(math.log(8.0) - 1.3862944 * jax.random.uniform(key_of[3], (NX2, NY, TILE), jnp.float32) ** level_of(key_of[3], (NX2, NY, TILE), ((0, 8), (1, 4)), -0.2, 0.2)), 2.0, 8.0)
    coupling = jnp.clip(jax.random.uniform(key_of[4], (PHASES, PHASES, NX2, NY, TILE), jnp.float32, -0.3, 0.3) * level_of(key_of[4], (PHASES, PHASES, NX2, NY, TILE), ((2, 8), (3, 4)), -0.4, 0.0), -0.3, 0.3)
    well_cells = set_ends(jax.random.randint(key_of[5], (N_WIDE, N_NARROW, CONN), 0, PX * CY * TILE), jax.random.fold_in(key_of[5], 1), 0, (PX * CY * TILE) - 1).astype(jnp.int32)
    well_index = jnp.clip(jnp.exp(math.log(20.0) - 2.9957323 * jax.random.uniform(key_of[6], (N_WIDE, N_NARROW, CONN), jnp.float32) ** level_of(key_of[6], (N_WIDE, N_NARROW, CONN), ((0, 8), (1, 4)), -0.2, 0.2)), 1.0, 20.0)
    agg_map = set_ends(jax.random.randint(key_of[7], (NX2, NY, TILE), 0, AGG_LOC), jax.random.fold_in(key_of[7], 1), 0, AGG_LOC - 1).astype(jnp.int32)
    tile_factors = draw_tile_factors(jax.random.fold_in(key_of[10], 71), 0)
    coarse_inverse = draw_coarse_inverse(jax.random.fold_in(key_of[10], 71), 0)
    return {"rhs": rhs, "start": start, "trans": trans, "accum": accum, "coupling": coupling, "well_cells": well_cells, "well_index": well_index, "agg_map": agg_map, "tile_factors": tile_factors, "coarse_inverse": coarse_inverse}


best_precision = lax.Precision.HIGHEST


def neighbour(values, along, offset, periodic):
    along = along % values.ndim
    if periodic:
        return jnp.roll(values, -offset, axis=along)
    length = values.shape[along]
    padding = [(0, 0)] * values.ndim
    if offset > 0:
        padding[along] = (0, offset)
        return lax.slice_in_dim(jnp.pad(values, padding), offset, offset + length, axis=along)
    padding[along] = (-offset, 0)
    return lax.slice_in_dim(jnp.pad(values, padding), 0, length, axis=along)


def east_of(values, periodic):
    middle = values.shape[-1] // 2
    from_next = neighbour(values, -3, 1, periodic)[..., :middle]
    return jnp.concatenate([values[..., middle:], from_next], axis=-1)


def west_of(values, periodic):
    middle = values.shape[-1] // 2
    from_prev = neighbour(values, -3, -1, periodic)[..., middle:]
    return jnp.concatenate([from_prev, values[..., :middle]], axis=-1)


def prepare(trans, accum_w, periodic):
    middle = trans.shape[-1] // 2
    layer_no = lax.broadcasted_iota(jnp.int32, accum_w.shape, accum_w.ndim - 1) % middle
    trans_x = trans[0]
    trans_y = trans[1]
    trans_z = jnp.where(layer_no < middle - 1, trans[2], 0.0)
    face_sum = trans_x + west_of(trans_x, periodic) + trans_y + neighbour(trans_y, -2, -1, periodic)
    face_sum = face_sum + trans_z + neighbour(trans_z, -1, -1, False)
    return trans_x, trans_y, trans_z, accum_w + face_sum


def operate(values, trans_x, trans_y, trans_z, centre, coupling, periodic):
    mixing = jnp.sum(coupling * values[None], axis=1)
    inflow = trans_x * east_of(values, periodic) + west_of(trans_x, periodic) * west_of(values, periodic)
    inflow = inflow + trans_y * neighbour(values, -2, 1, periodic)
    inflow = inflow + neighbour(trans_y, -2, -1, periodic) * neighbour(values, -2, -1, periodic)
    inflow = inflow + trans_z * neighbour(values, -1, 1, False)
    inflow = inflow + neighbour(trans_z, -1, -1, False) * neighbour(values, -1, -1, False)
    return centre * values + mixing - inflow


def tile_apply(values, inverse_diag, factors):
    scaled = (inverse_diag * values).astype(jnp.bfloat16)
    return jnp.einsum("cpyj,pykj->cpyk", scaled.astype(jnp.float32), factors.astype(jnp.float32), precision=best_precision)


def local_solve(misfit, coeffs, inverse_diag, factors):
    trans_x, trans_y, trans_z, centre, coupling = coeffs
    update = tile_apply(misfit, inverse_diag, factors)
    for _ in range(INNER - 1):
        applied = operate(update, trans_x, trans_y, trans_z, centre, coupling, False)
        update = update + tile_apply(misfit - applied, inverse_diag, factors)
    return update


def wrap_pad(values):
    widths = ((1, 1), (2, 2), (0, 0))
    return jnp.pad(values, ((0, 0),) * (values.ndim - 3) + widths, mode="wrap")


def subdomains(misfit_pad, padded, tile_factors):
    def one_device(device_no):
        wide_pos = (device_no // N_NARROW).astype(jnp.int32)
        narrow_pos = (device_no % N_NARROW).astype(jnp.int32)
        zero = jnp.zeros((), jnp.int32)

        def window(values):
            cut_x = lax.dynamic_slice_in_dim(values, (wide_pos * PX).astype(jnp.int32), PX + 2, values.ndim - 3)
            return lax.dynamic_slice_in_dim(cut_x, (narrow_pos * CY).astype(jnp.int32), CY + 4, values.ndim - 2)

        coeffs = [window(member) for member in padded[:5]]
        starts = ((wide_pos * (PX + 2)).astype(jnp.int32), (narrow_pos * (CY + 4)).astype(jnp.int32), zero, zero)
        factors = lax.dynamic_slice(tile_factors, starts, (PX + 2, CY + 4, TILE, TILE))
        update = local_solve(window(misfit_pad), coeffs, window(padded[5]), factors)
        return update[:, 1:-1, 2:-2, :]

    blocks = lax.map(one_device, jnp.arange(N_WIDE * N_NARROW, dtype=jnp.int32))
    blocks = blocks.reshape(N_WIDE, N_NARROW, PHASES, PX, CY, TILE)
    return blocks.transpose(2, 0, 3, 1, 4, 5).reshape(PHASES, N_WIDE * PX, N_NARROW * CY, TILE)


def reference(rhs, start, trans, accum, coupling, well_cells, well_index, agg_map, tile_factors, coarse_inverse):
    flat_local = well_cells.astype(jnp.int32)
    pair_pos = jnp.arange(N_WIDE, dtype=jnp.int32)[:, None, None] * PX + flat_local // (CY * TILE)
    row_pos = jnp.arange(N_NARROW, dtype=jnp.int32)[None, :, None] * CY + (flat_local // TILE) % CY
    cell_pos = flat_local % TILE
    accum_w = accum.at[pair_pos, row_pos, cell_pos].add(well_index)
    trans_x, trans_y, trans_z, centre = prepare(trans, accum_w, True)
    coupling_diag = jnp.stack([coupling[member, member] for member in range(PHASES)])
    inverse_diag = 1.0 / (centre[None] + coupling_diag)
    padded = [wrap_pad(member) for member in (trans_x, trans_y, trans_z, centre, coupling, inverse_diag)]
    owner_no = (lax.broadcasted_iota(jnp.int32, accum.shape, 0) // PX) * N_NARROW
    owner_no = owner_no + lax.broadcasted_iota(jnp.int32, accum.shape, 1) // CY
    group_ids = (owner_no * AGG_LOC + agg_map.astype(jnp.int32)).reshape(-1)
    current = start
    for _ in range(SWEEPS):
        misfit = rhs - operate(current, trans_x, trans_y, trans_z, centre, coupling, True)
        correction = subdomains(wrap_pad(misfit), padded, tile_factors)
        coarse_rhs = jax.ops.segment_sum(misfit[0].reshape(-1), group_ids, num_segments=NAGG)
        coarse_sol = jnp.dot(coarse_inverse, coarse_rhs, precision=best_precision)
        correction = correction.at[0].add(coarse_sol[group_ids].reshape(accum.shape))
        current = current + correction
    final_misfit = rhs - operate(current, trans_x, trans_y, trans_z, centre, coupling, True)
    return current, final_misfit
```

```python
import jax
import jax.numpy as jnp
from jax import lax
from jax.sharding import PartitionSpec as P

AGG_LOC = 32
SWEEPS = 3
INNER = 3


best_precision = lax.Precision.HIGHEST


def halos(tail, head, axis):
    count = lax.axis_size(axis)
    if count % 2:
        low = lax.ppermute(tail, axis, [(i, (i + 1) % count) for i in range(count)])
        high = lax.ppermute(head, axis, [((i + 1) % count, i) for i in range(count)])
        return low, high
    even = lax.axis_index(axis) % 2 == 0
    first = lax.ppermute(jnp.where(even, tail, head), axis, [(i, i ^ 1) for i in range(count)])
    other = [(i, (i - 1 if i % 2 == 0 else i + 1) % count) for i in range(count)]
    second = lax.ppermute(jnp.where(even, head, tail), axis, other)
    return jnp.where(even, second, first), jnp.where(even, first, second)


def padded(cells, sides, width):
    for axis, dim in sides:
        head = lax.slice_in_dim(cells, 0, width, axis=dim)
        tail = lax.slice_in_dim(cells, cells.shape[dim] - width, cells.shape[dim], axis=dim)
        low, high = halos(tail, head, axis)
        cells = jnp.concatenate([low, cells, high], axis=dim)
    return cells


def neighbour(values, along, offset):
    along = along % values.ndim
    length = values.shape[along]
    padding = [(0, 0)] * values.ndim
    if offset > 0:
        padding[along] = (0, offset)
        return lax.slice_in_dim(jnp.pad(values, padding), offset, offset + length, axis=along)
    padding[along] = (-offset, 0)
    return lax.slice_in_dim(jnp.pad(values, padding), 0, length, axis=along)


def east_of(values):
    middle = values.shape[-1] // 2
    from_next = neighbour(values, -3, 1)[..., :middle]
    return jnp.concatenate([values[..., middle:], from_next], axis=-1)


def west_of(values):
    middle = values.shape[-1] // 2
    from_prev = neighbour(values, -3, -1)[..., middle:]
    return jnp.concatenate([from_prev, values[..., :middle]], axis=-1)


def prepare(trans, accum_w):
    middle = trans.shape[-1] // 2
    layer_no = lax.broadcasted_iota(jnp.int32, accum_w.shape, accum_w.ndim - 1) % middle
    trans_x = trans[0]
    trans_y = trans[1]
    trans_z = jnp.where(layer_no < middle - 1, trans[2], 0.0)
    face_sum = trans_x + west_of(trans_x) + trans_y + neighbour(trans_y, -2, -1)
    face_sum = face_sum + trans_z + neighbour(trans_z, -1, -1)
    return (trans_x, trans_y, trans_z, accum_w + face_sum)


def operate(values, trans_x, trans_y, trans_z, centre, coupling):
    mixing = jnp.sum(coupling * values[None], axis=1)
    inflow = trans_x * east_of(values) + west_of(trans_x) * west_of(values)
    inflow = inflow + trans_y * neighbour(values, -2, 1)
    inflow = inflow + neighbour(trans_y, -2, -1) * neighbour(values, -2, -1)
    inflow = inflow + trans_z * neighbour(values, -1, 1)
    inflow = inflow + neighbour(trans_z, -1, -1) * neighbour(values, -1, -1)
    return centre * values + mixing - inflow


def tile_apply(values, inverse_diag, factors):
    scaled = (inverse_diag * values).astype(jnp.bfloat16)
    return jnp.einsum("cpyj,pykj->cpyk", scaled, factors, preferred_element_type=jnp.float32)


def local_solve(misfit, coeffs, inverse_diag, factors):
    trans_x, trans_y, trans_z, centre, coupling = coeffs
    update = tile_apply(misfit, inverse_diag, factors)
    for _ in range(INNER - 1):
        applied = operate(update, trans_x, trans_y, trans_z, centre, coupling)
        update = update + tile_apply(misfit - applied, inverse_diag, factors)
    return update


def per_device(
    rhs,
    start,
    trans,
    accum,
    coupling,
    well_cells,
    well_index,
    agg_map,
    tile_factors,
    coarse_inverse,
):
    phases = rhs.shape[0]
    devices = lax.axis_size("wide") * lax.axis_size("narrow")
    accum_flat = accum.reshape(-1).at[well_cells.reshape(-1)].add(well_index.reshape(-1))
    accum_w = accum_flat.reshape(accum.shape)
    stacked = jnp.concatenate(
        [trans, accum_w[None], coupling.reshape((phases * phases,) + accum.shape)], axis=0
    )
    stacked = jnp.concatenate([stacked, rhs], axis=0)
    rim_wide = padded(stacked, (("wide", 1),), 2)
    rim_full = padded(rim_wide, (("narrow", 2),), 3)
    trans_x, trans_y, trans_z, centre = prepare(rim_full[0:3], rim_full[3])
    coupling_full = rim_full[4:13].reshape((phases, phases) + rim_full.shape[1:])
    full_set = (trans_x, trans_y, trans_z, centre, coupling_full)
    ext_set = tuple((member[..., 1:-1, 1:-1, :] for member in full_set))
    diag_part = jnp.stack([ext_set[4][member, member] for member in range(phases)])
    inverse_diag = 1.0 / (ext_set[3][None] + diag_part)

    def extended_fn(current):
        rim_x = padded(current, (("wide", 1),), 2)
        rim_xy = padded(rim_x, (("narrow", 2),), 3)
        applied = operate(rim_xy, full_set[0], full_set[1], full_set[2], full_set[3], full_set[4])
        extended = (rim_full[13:] - applied)[..., 1:-1, 1:-1, :]
        return (extended, extended[..., 1:-1, 2:-2, :])

    groups = jnp.arange(AGG_LOC, dtype=jnp.int32)
    member_of = (groups[:, None] == agg_map.reshape(1, -1)).astype(jnp.float32)
    current = start
    for _ in range(SWEEPS):
        extended, owned_misfit = extended_fn(current)
        coarse_rhs = jnp.dot(member_of, owned_misfit[0].reshape(-1), precision=best_precision)
        copies = jnp.broadcast_to(coarse_rhs, (devices,) + coarse_rhs.shape)
        coarse_all = lax.all_to_all(copies, ("wide", "narrow"), 0, 0, tiled=True).reshape(-1)
        coarse_sol = jnp.dot(coarse_inverse, coarse_all, precision=best_precision)
        update = local_solve(extended, ext_set, inverse_diag, tile_factors)[..., 1:-1, 2:-2, :]
        lifted = jnp.dot(coarse_sol, member_of, precision=best_precision).reshape(accum.shape)
        current = current + update.at[0].add(lifted)
    final_misfit = extended_fn(current)[1]
    return (current, final_misfit)


def solution(mesh):
    return jax.shard_map(
        per_device,
        mesh=mesh,
        in_specs=(
            P(None, "wide", "narrow", None),
            P(None, "wide", "narrow", None),
            P(None, "wide", "narrow", None),
            P("wide", "narrow", None),
            P(None, None, "wide", "narrow", None),
            P("wide", "narrow", None),
            P("wide", "narrow", None),
            P("wide", "narrow", None),
            P("wide", "narrow", None, None),
            P(("wide", "narrow"), None),
        ),
        out_specs=(P(None, "wide", "narrow", None), P(None, "wide", "narrow", None)),
        check_vma=False,
    )
```

```python
import functools

import jax
import jax.numpy as jnp
from jax import lax
from jax.experimental import pallas as pl
from jax.experimental.pallas import tpu as pltpu
from jax.sharding import PartitionSpec as P

AGG_LOC = 32
SWEEPS = 3
INNER = 3
HX = 2
HY = 3

TX, TY, TZ, ACC, CPL, RHS, CUR, IDX, FIELDS = 0, 1, 2, 3, 4, 13, 16, 19, 20
OUTER_X = (TX, CUR, CUR + 1, CUR + 2, IDX)
OUTER_Y = (TY, CUR, CUR + 1, CUR + 2, IDX)
GC, GI, GR, GFIELDS = 3, 12, 15, 18

PARAMS = pltpu.CompilerParams(vmem_limit_bytes=16 * 1024 * 1024)


HBM = pl.BlockSpec(memory_space=pltpu.HBM)
VMEM = pl.BlockSpec(memory_space=pltpu.VMEM)


def call(body, outs, scratch=(), far=(), far_outs=()):
    def run(flags, *args):
        specs = [pl.BlockSpec(memory_space=pltpu.SMEM)]
        specs += [HBM if number in far else VMEM for number in range(len(args))]
        args = [
            pltpu.with_memory_space_constraint(arg, pltpu.HBM) if number in far else arg
            for number, arg in enumerate(args)
        ]
        return pl.pallas_call(
            body,
            out_shape=tuple(
                (pltpu.HBM if number in far_outs else jax.ShapeDtypeStruct)(*out) for number, out in enumerate(outs)
            ),
            in_specs=specs,
            out_specs=tuple(HBM if number in far_outs else VMEM for number in range(len(outs))),
            scratch_shapes=list(scratch),
            compiler_params=PARAMS,
            name=body.func.__name__ if isinstance(body, functools.partial) else body.__name__,
        )(flags, *args)

    return run


def rows_of(ref):
    size = 1
    for length in ref.shape[:-1]:
        size *= length
    return ref.reshape(size, ref.shape[-1])


def sent(flags, axis, tail, head):
    low_first = flags[2 * axis] == 0
    return jnp.where(low_first, tail, head), jnp.where(low_first, head, tail)


def received(flags, axis, first, second):
    swapped = flags[2 * axis + 1] == 0
    return jnp.where(swapped, second, first), jnp.where(swapped, first, second)


def split3(values):
    high = values.astype(jnp.bfloat16)
    rest = values - high.astype(jnp.float32)
    middle = rest.astype(jnp.bfloat16)
    low = (rest - middle.astype(jnp.float32)).astype(jnp.bfloat16)
    return high, middle, low


def nt_dot(left, right):
    return lax.dot_general(left, right, (((1,), (1,)), ((), ())), preferred_element_type=jnp.float32)


def pack_wide(flags, trans, accum, coupling, rhs, start, agg, far_cells, far_index, block, first, second, groups, cells, index, sems):
    phases, px, cy, tile = rhs.shape
    conn = cells.shape[-1]
    copies = [
        (far_cells, cells),
        (far_index, index),
        (accum, block.at[ACC]),
        (agg, groups),
        (trans, block.at[pl.ds(TX, 3)]),
        (rhs, block.at[pl.ds(RHS, phases)]),
        (start, block.at[pl.ds(CUR, phases)]),
    ]
    copies += [(coupling.at[c], block.at[pl.ds(CPL + c * phases, phases)]) for c in range(phases)]
    copies = [pltpu.make_async_copy(source, target, sems.at[k]) for k, (source, target) in enumerate(copies)]
    for copy in copies:
        copy.start()
    for copy in copies[:2]:
        copy.wait()
    where_to = cells[0]
    row_no = lax.broadcasted_iota(jnp.int32, (px * cy, conn), 0)
    lane_no = lax.broadcasted_iota(jnp.int32, (tile, conn), 0)
    lanes = jnp.where(lane_no == where_to % tile, 1.0, 0.0).astype(jnp.bfloat16)
    rows = jnp.where(row_no == where_to // tile, index[0], 0.0)
    added = sum(nt_dot(part, lanes) for part in split3(rows))
    for copy in copies[2:]:
        copy.wait()
    for pair in range(px):
        block[ACC, pair] = block[ACC, pair] + added[pair * cy : (pair + 1) * cy]
        block[IDX, pair] = (groups[pair] + flags[4]).astype(jnp.float32)
    for number in range(FIELDS):
        one, two = sent(flags, 0, block[number, px - 1], block[number, 0])
        first[number] = one
        second[number] = two
    for place, number in enumerate(OUTER_X):
        one, two = sent(flags, 0, block[number, px - 2], block[number, 1])
        first[FIELDS + place] = one
        second[FIELDS + place] = two


def pack_narrow(flags, block, got_first, got_second, own, first, second):
    px, cy, tile = block.shape[1:]
    width = px + 2 * HX
    own_rows = rows_of(own)

    def put(number, pair, values):
        own_rows[pl.ds(number * cy * width + pair, cy, stride=width), :] = values

    for number in range(FIELDS):
        low, high = received(flags, 0, got_first[number], got_second[number])
        put(number, HX - 1, low)
        put(number, HX + px, high)
        if number in OUTER_X:
            place = FIELDS + OUTER_X.index(number)
            low, high = received(flags, 0, got_first[place], got_second[place])
        else:
            low = high = jnp.zeros((cy, tile), jnp.float32)
        put(number, 0, low)
        put(number, width - 1, high)
        for pair in range(px):
            put(number, HX + pair, block[number, pair])
    for number in range(FIELDS):
        for column in range(HY - 1):
            one, two = sent(flags, 1, own[number, cy - HY + 1 + column], own[number, column])
            first[number * (HY - 1) + column] = one
            second[number * (HY - 1) + column] = two
    for place, number in enumerate(OUTER_Y):
        one, two = sent(flags, 1, own[number, cy - HY], own[number, HY - 1])
        first[FIELDS * (HY - 1) + place] = one
        second[FIELDS * (HY - 1) + place] = two


def lane_half(shape):
    return lax.broadcasted_iota(jnp.int32, shape, len(shape) - 1) < shape[-1] // 2


def swap_half(values):
    return pltpu.roll(values, values.shape[-1] // 2, values.ndim - 1)


def east_of(values, half):
    turned = swap_half(values)
    return jnp.where(half, turned, pltpu.roll(turned, values.shape[-2] - 1, values.ndim - 2))


def west_of(values, half):
    turned = swap_half(values)
    return jnp.where(half, pltpu.roll(turned, 1, values.ndim - 2), turned)


def above(values):
    return pltpu.roll(values, values.shape[-1] - 1, values.ndim - 1)


def below(values):
    return pltpu.roll(values, 1, values.ndim - 1)


def operate(field, coeffs, column, half):
    phases = 3
    here = [field(c, column) for c in range(phases)]
    tx, ty, tz = coeffs[0, column], coeffs[1, column], coeffs[2, column]
    ty_before = coeffs[1, column - 1]
    results = []
    for c in range(phases):
        value = here[c]
        mixed = sum(coeffs[GC + c * phases + b, column] * here[b] for b in range(phases))
        inflow = tx * east_of(value, half) + west_of(tx * value, half)
        inflow = inflow + (ty * field(c, column + 1) + ty_before * field(c, column - 1))
        inflow = inflow + (tz * above(value) + below(tz * value))
        results.append(mixed - inflow)
    return results


def coarse_share(own_misfit, agg_rows, cinv, share, slots, px, cy, narrow):
    count, total = cinv.shape
    lanes = total // share.shape[0]
    width = px + 2 * HX
    agg_no = lax.broadcasted_iota(jnp.int32, (count, own_misfit.shape[-1]), 0)
    parts = [jnp.zeros(agg_no.shape, jnp.float32) for _ in range(4)]
    for column in range(cy):
        for pair in range(px):
            row = column * width + HX + pair
            here = agg_rows[pl.ds(row, 1), :]
            value = own_misfit[pl.ds(row, 1), :]
            spot = (column * px + pair) % len(parts)
            parts[spot] = parts[spot] + jnp.where(agg_no == here, value, 0.0)
    sums = jnp.sum((parts[0] + parts[1]) + (parts[2] + parts[3]), axis=1, keepdims=True)
    wide = share.shape[0]
    for i in range(wide):
        share[pl.ds(i, 1), :] = jnp.sum(cinv[:, i * lanes : (i + 1) * lanes] * sums, axis=0, keepdims=True)
    pair_no = lax.broadcasted_iota(jnp.int32, (width, lanes), 0)
    for i in range(wide):
        before = share[pl.ds((i - 1) % wide, 1), :]
        here = share[pl.ds(i, 1), :]
        after = share[pl.ds((i + 1) % wide, 1), :]
        table = jnp.where(pair_no < HX, before, jnp.where(pair_no < HX + px, here, after))
        for j in range(narrow):
            slots[i * narrow + j] = table


def misfit_and_share(flags, coeffs, current, misfit, index, cinv, slots, own_misfit, own_agg, share, px, cy, narrow):
    columns = current.shape[1]
    half = lane_half(current.shape[2:])
    for column in range(1, columns - 1):
        applied = operate(lambda c, y: current[c, y], coeffs, column, half)
        for c in range(3):
            value = coeffs[GR + c, column] - applied[c]
            misfit[c, column] = value
            if c == 0 and HY <= column < HY + cy:
                own_misfit[column - HY] = value
    for column in range(cy):
        own_agg[column] = index[HY + column] - flags[4]
    coarse_share(rows_of(own_misfit), rows_of(own_agg), cinv, share, slots, px, cy, narrow)


def sweep_body(flags, coeffs, current, index, cinv, hot, factors, update, slots, first, second, px, narrow, scratch):
    misfit, work, hold, own_misfit, own_agg, share, near_slots, cold, sems = scratch
    cy = update.shape[1]
    edge = HY - 1
    boxes = factors.shape[1]
    loads = [
        pltpu.make_async_copy(factors.at[:, pl.ds(0, edge)], cold.at[:, pl.ds(0, edge)], sems.at[0]),
        pltpu.make_async_copy(factors.at[:, pl.ds(boxes - edge, edge)], cold.at[:, pl.ds(edge, edge)], sems.at[1]),
    ]
    for load in loads:
        load.start()
    misfit_and_share(flags, coeffs, current, misfit, index, cinv, near_slots, own_misfit, own_agg, share, px, cy, narrow)
    send = pltpu.make_async_copy(near_slots, slots, sems.at[2])
    send.start()
    solve(flags, misfit, coeffs, hot, cold, loads, update, first, second, work, hold)
    send.wait()


def prepare(flags, own, got_first, got_second, cinv, hot, factors, coeffs, index, current, update, slots, first, second, field, *scratch, px, narrow):
    cy = own.shape[1]
    columns = cy + 2 * HY
    half = lane_half(own.shape[2:])
    depth = lax.broadcasted_iota(jnp.int32, own.shape[2:], 1) % (own.shape[3] // 2)
    for number in range(FIELDS):
        for column in range(cy):
            field[number, HY + column] = own[number, column]
        for column in range(HY - 1):
            low, high = received(
                flags, 1, got_first[number * (HY - 1) + column], got_second[number * (HY - 1) + column]
            )
            field[number, 1 + column] = low
            field[number, HY + cy + column] = high
    for place, number in enumerate(OUTER_Y):
        place = FIELDS * (HY - 1) + place
        low, high = received(flags, 1, got_first[place], got_second[place])
        field[number, 0] = low
        field[number, columns - 1] = high
    for column in range(columns):
        index[column] = field[IDX, column].astype(jnp.int32)
        for c in range(3):
            current[c, column] = field[CUR + c, column]
    coeffs[1, 0] = field[TY, 0]
    for column in range(1, columns - 1):
        tx, ty = field[TX, column], field[TY, column]
        tz = jnp.where(depth < own.shape[3] // 2 - 1, field[TZ, column], 0.0)
        faces = (tx + west_of(tx, half)) + (ty + field[TY, column - 1]) + (tz + below(tz))
        centre = field[ACC, column] + faces
        coeffs[0, column] = tx
        coeffs[1, column] = ty
        coeffs[2, column] = tz
        for number in range(9):
            value = field[CPL + number, column]
            if number % 4 == 0:
                value = value + centre
                coeffs[GI + number // 4, column] = 1.0 / value
            coeffs[GC + number, column] = value
        for c in range(3):
            coeffs[GR + c, column] = field[RHS + c, column]
    sweep_body(flags, coeffs, current, index, cinv, hot, factors, update, slots, first, second, px, narrow, scratch)


def tile_apply(values, coeffs, tiles, column, first, last):
    scaled = [coeffs[GI + c, column] * values[c] for c in range(3)]
    stacked = jnp.concatenate(scaled, axis=0)
    width = scaled[0].shape[0]
    pair_no = lax.broadcasted_iota(jnp.int32, stacked.shape, 0) % width
    left = [jnp.where(pair_no == a + HX - 1, stacked, 0.0).astype(jnp.bfloat16) for a in range(first, last)]
    right = [tiles(a, column - 1) for a in range(first, last)]
    result = nt_dot(jnp.concatenate(left, axis=1), jnp.concatenate(right, axis=1))
    return [result[c * width : (c + 1) * width] for c in range(3)]


def solve(flags, misfit, coeffs, hot, cold, loads, update, first, second, work, hold):
    phases, columns = work.shape[:2]
    cy = columns - 2 * HY
    boxes = hot.shape[0]
    width = work.shape[2]
    px = width - 2 * HX
    edge = HY - 1
    half = lane_half(work.shape[2:])

    def tiles(a, b):
        if b < edge:
            return cold[a, b]
        return hot[a, b - edge] if b < edge + cy else cold[a, b - cy]

    for c in range(phases):
        work[c, 0] = jnp.zeros(work.shape[2:], jnp.float32)
        work[c, columns - 1] = jnp.zeros(work.shape[2:], jnp.float32)
    inside = list(range(HY, HY + cy))
    outside = [column for column in range(1, columns - 1) if column not in inside]
    for column in inside + outside:
        if column == outside[0]:
            for load in loads:
                load.wait()
        new = tile_apply([misfit[c, column] for c in range(phases)], coeffs, tiles, column, 0, boxes)
        for c in range(phases):
            work[c, column] = new[c]
    for step in range(1, INNER):
        spare = max(HY - 1 - (INNER - 1 - step), 0)
        needed = range(1 + spare, columns - 1 - spare)
        last = step == INNER - 1
        first_box, last_box = (1, boxes - 1) if last else (0, boxes)
        for column in needed:
            applied = operate(lambda c, y: work[c, y], coeffs, column, half)
            left = [misfit[c, column] - applied[c] for c in range(phases)]
            new = tile_apply(left, coeffs, tiles, column, first_box, last_box)
            for c in range(phases):
                hold[c, column] = work[c, column] + new[c]
        for column in needed:
            for c in range(phases):
                if last:
                    update[c, column - HY] = hold[c, column]
                else:
                    work[c, column] = hold[c, column]
    rows = rows_of(update)
    for c in range(phases):
        for pair in range(HX):
            tail = rows[pl.ds(c * cy * width + px + pair, cy, stride=width), :]
            head = rows[pl.ds(c * cy * width + HX + pair, cy, stride=width), :]
            one, two = sent(flags, 0, tail, head)
            first[c, pair] = one
            second[c, pair] = two


def widen(flags, update, got_first, got_second, whole, first, second):
    phases, cy, width, _ = update.shape
    px = width - 2 * HX
    whole[...] = update[...]
    rows = rows_of(whole)
    for c in range(phases):
        for pair in range(HX):
            low, high = received(flags, 0, got_first[c, pair], got_second[c, pair])
            rows[pl.ds(c * cy * width + pair, cy, stride=width), :] = low
            rows[pl.ds(c * cy * width + HX + px + pair, cy, stride=width), :] = high
    for c in range(phases):
        for column in range(HY):
            one, two = sent(flags, 1, whole[c, cy - HY + column], whole[c, column])
            first[c, column] = one
            second[c, column] = two


def advance(flags, current, index, whole, got_first, got_second, slots_in, result):
    phases, columns = current.shape[:2]
    cy = columns - 2 * HY
    total = [slots_in[d] for d in range(min(4, slots_in.shape[0]))]
    for d in range(4, slots_in.shape[0]):
        total[d % 4] = total[d % 4] + slots_in[d]
    table = sum(total[1:], total[0])
    for column in range(columns):
        for c in range(phases):
            if column < HY:
                change = received(flags, 1, got_first[c, column], got_second[c, column])[0]
            elif column < HY + cy:
                change = whole[c, column - HY]
            else:
                place = column - HY - cy
                change = received(flags, 1, got_first[c, place], got_second[c, place])[1]
            value = current[c, column] + change
            if c == 0:
                value = value + jnp.take_along_axis(table, index[column], axis=1)
            result[c, column] = value


def next_sweep(flags, current, coeffs, index, whole, got_first, got_second, slots_in, cinv, hot, factors, result, update, slots, first, second, *scratch, px, narrow):
    advance(flags, current, index, whole, got_first, got_second, slots_in, result)
    sweep_body(flags, coeffs, result, index, cinv, hot, factors, update, slots, first, second, px, narrow, scratch)


def finish(flags, current, coeffs, index, whole, got_first, got_second, slots_in, iterate, residual, result, misfit):
    advance(flags, current, index, whole, got_first, got_second, slots_in, result)
    phases, px, cy, _ = iterate.shape
    columns, width = current.shape[1:3]
    half = lane_half(current.shape[2:])
    for column in range(HY, HY + cy):
        applied = operate(lambda c, y: result[c, y], coeffs, column, half)
        for c in range(phases):
            misfit[c, column] = coeffs[GR + c, column] - applied[c]
    for source, target in ((rows_of(result), iterate), (rows_of(misfit), residual)):
        for c in range(phases):
            for pair in range(px):
                target[c, pair] = source[pl.ds((c * columns + HY) * width + HX + pair, cy, stride=width), :]


def swap(first, second, axis):
    count = lax.axis_size(axis)
    if count % 2:
        pairs = [[(i, (i + 1) % count) for i in range(count)], [((i + 1) % count, i) for i in range(count)]]
    else:
        pairs = [
            [(i, i ^ 1) for i in range(count)],
            [(i, (i + 1 if i % 2 else i - 1) % count) for i in range(count)],
        ]
    return lax.ppermute(first, axis, pairs[0]), lax.ppermute(second, axis, pairs[1])


def order_flags():
    flags = []
    for axis in ("wide", "narrow"):
        place = lax.axis_index(axis) % 2
        odd = lax.axis_size(axis) % 2
        flags += [0, 1] if odd else [place, place]
    return jnp.stack([jnp.asarray(flag, jnp.int32) for flag in flags + [lax.axis_index("narrow") * AGG_LOC]])


def per_device(
    rhs,
    start,
    trans,
    accum,
    coupling,
    well_cells,
    well_index,
    agg_map,
    tile_factors,
    coarse_inverse,
):
    phases, px, cy, tile = rhs.shape
    wide, narrow = lax.axis_size("wide"), lax.axis_size("narrow")
    width, columns = px + 2 * HX, cy + 2 * HY
    f32 = jnp.float32
    flags = order_flags()
    lanes = narrow * AGG_LOC

    face = ((FIELDS + len(OUTER_X), cy, tile), f32)
    block, first, second = call(
        pack_wide,
        [((FIELDS, px, cy, tile), f32), face, face],
        [
            pltpu.VMEM((px, cy, tile), jnp.int32),
            pltpu.VMEM(well_cells.shape, jnp.int32),
            pltpu.VMEM(well_index.shape, f32),
            pltpu.SemaphoreType.DMA((7 + phases,)),
        ],
        far=range(8),
    )(flags, trans, accum, coupling, rhs, start, agg_map, well_cells, well_index)
    first, second = swap(first, second, "wide")
    face = ((FIELDS * (HY - 1) + len(OUTER_Y), width, tile), f32)
    own, first, second = call(pack_narrow, [((FIELDS, cy, width, tile), f32), face, face])(
        flags, block, first, second
    )
    first, second = swap(first, second, "narrow")

    vec = (width, tile)
    field = ((phases, columns) + vec, f32)
    inner = ((phases, columns - 1) + vec, f32)
    slot = ((wide * narrow, width, lanes), f32)
    part = ((phases, cy) + vec, f32)
    face = ((phases, HX, cy, tile), f32)
    edge_face = ((phases, HY) + vec, f32)
    boxes = tile_factors.shape
    scratch = [
        pltpu.VMEM(*inner),
        pltpu.VMEM(*field),
        pltpu.VMEM(*field),
        pltpu.VMEM((cy,) + vec, f32),
        pltpu.VMEM((cy,) + vec, jnp.int32),
        pltpu.VMEM((wide, lanes), f32),
        pltpu.VMEM(*slot),
        pltpu.VMEM((boxes[0], 2 * (HY - 1)) + boxes[2:], tile_factors.dtype),
        pltpu.SemaphoreType.DMA((3,)),
    ]
    hot = tile_factors[:, HY - 1 : HY - 1 + cy]
    coeffs, index, current, update, slots, first, second = call(
        functools.partial(prepare, px=px, narrow=narrow),
        [((GFIELDS, columns - 1) + vec, f32), ((columns,) + vec, jnp.int32), field, part, slot, face, face],
        [pltpu.VMEM((FIELDS, columns) + vec, f32)] + scratch,
        far=(5,),
        far_outs=(4,),
    )(flags, own, first, second, coarse_inverse, hot, tile_factors)
    for sweep in range(SWEEPS):
        gathered = lax.all_to_all(slots, ("wide", "narrow"), 0, 0, tiled=True)
        first, second = swap(first, second, "wide")
        whole, first, second = call(widen, [part, edge_face, edge_face])(flags, update, first, second)
        first, second = swap(first, second, "narrow")
        if sweep < SWEEPS - 1:
            current, update, slots, first, second = call(
                functools.partial(next_sweep, px=px, narrow=narrow),
                [field, part, slot, face, face],
                scratch,
                far=(9,),
                far_outs=(2,),
            )(flags, current, coeffs, index, whole, first, second, gathered, coarse_inverse, hot, tile_factors)
    out = (rhs.shape, f32)
    return call(finish, [out, out], [pltpu.VMEM(*field), pltpu.VMEM(*field)])(
        flags, current, coeffs, index, whole, first, second, gathered
    )


def solution(mesh):
    return jax.shard_map(
        per_device,
        mesh=mesh,
        in_specs=(
            P(None, "wide", "narrow", None),
            P(None, "wide", "narrow", None),
            P(None, "wide", "narrow", None),
            P("wide", "narrow", None),
            P(None, None, "wide", "narrow", None),
            P("wide", "narrow", None),
            P("wide", "narrow", None),
            P("wide", "narrow", None),
            P("wide", "narrow", None, None),
            P(("wide", "narrow"), None),
        ),
        out_specs=(P(None, "wide", "narrow", None), P(None, "wide", "narrow", None)),
        check_vma=False,
    )
```

```python
import functools

import jax
import jax.numpy as jnp
from jax import lax
from jax.experimental import pallas as pl
from jax.experimental.pallas import tpu as pltpu
from jax.sharding import PartitionSpec as P

AGG_LOC = 32
SWEEPS = 3
HX = 2
HY = 3

TX, TY, TZ, CPL, RHS, CUR, IDX, FIELDS = 0, 1, 2, 3, 12, 15, 18, 19
OUTER_X = (TX, CUR, CUR + 1, CUR + 2, IDX)
OUTER_Y = (TY, CUR, CUR + 1, CUR + 2, IDX)
CORNERS = ((-1, -1), (-1, 1), (1, -1), (1, 1))
CORNER_TILES = ((1, 1), (1, 2), (2, 1))
COLD = 2
SLOT = (3, 4)
GC, GI, GR, GFIELDS = 3, 12, 15, 18

PARAMS = pltpu.CompilerParams(vmem_limit_bytes=16 * 1024 * 1024)


HBM = pl.BlockSpec(memory_space=pltpu.HBM)
VMEM = pl.BlockSpec(memory_space=pltpu.VMEM)


def call(body, outs, scratch=(), far=(), far_outs=()):
    def run(flags, *args):
        specs = [pl.BlockSpec(memory_space=pltpu.SMEM)]
        specs += [HBM if number in far else VMEM for number in range(len(args))]
        args = [
            pltpu.with_memory_space_constraint(arg, pltpu.HBM) if number in far else arg
            for number, arg in enumerate(args)
        ]
        return pl.pallas_call(
            body,
            out_shape=tuple(
                (pltpu.HBM if number in far_outs else jax.ShapeDtypeStruct)(*out) for number, out in enumerate(outs)
            ),
            in_specs=specs,
            out_specs=tuple(HBM if number in far_outs else VMEM for number in range(len(outs))),
            scratch_shapes=list(scratch),
            compiler_params=PARAMS,
        )(flags, *args)

    return run


def rows_of(ref):
    size = 1
    for length in ref.shape[:-1]:
        size *= length
    return ref.reshape(size, ref.shape[-1])


def sent(flags, axis, tail, head):
    low_first = flags[2 * axis] == 0
    return jnp.where(low_first, tail, head), jnp.where(low_first, head, tail)


def received(flags, axis, first, second):
    swapped = flags[2 * axis + 1] == 0
    return jnp.where(swapped, second, first), jnp.where(swapped, first, second)


def split3(values):
    high = values.astype(jnp.bfloat16)
    rest = values - high.astype(jnp.float32)
    middle = rest.astype(jnp.bfloat16)
    low = (rest - middle.astype(jnp.float32)).astype(jnp.bfloat16)
    return high, middle, low


def nt_dot(left, right):
    return lax.dot_general(left, right, (((1,), (1,)), ((), ())), preferred_element_type=jnp.float32)


def fetch(flags, factors, after, *refs):
    *near, sems = refs
    cold = near[0]
    side = cold.shape[1] // 2
    inside = factors.shape[1] - 2 * side
    copies = [
        (factors.at[:, pl.ds(0, side)], cold.at[:, pl.ds(0, side)]),
        (factors.at[:, pl.ds(side + inside, side)], cold.at[:, pl.ds(side, side)]),
    ]
    copies += [(factors.at[:, pl.ds(side, inside)], hot) for hot in near[1:]]
    copies = [pltpu.make_async_copy(source, target, sems.at[k]) for k, (source, target) in enumerate(copies)]
    for copy in copies:
        copy.start()
    for copy in copies:
        copy.wait()


def pack_wide(flags, trans, accum, coupling, rhs, start, agg, far_cells, far_index, block, first, second, groups, near_accum, cells, index, sems):
    phases, px, cy, tile = rhs.shape
    conn = cells.shape[-1]
    copies = [
        (far_cells, cells),
        (far_index, index),
        (accum, near_accum),
        (agg, groups),
        (trans, block.at[pl.ds(TX, 3)]),
        (rhs, block.at[pl.ds(RHS, phases)]),
        (start, block.at[pl.ds(CUR, phases)]),
    ]
    copies += [(coupling.at[c], block.at[pl.ds(CPL + c * phases, phases)]) for c in range(phases)]
    copies = [pltpu.make_async_copy(source, target, sems.at[k]) for k, (source, target) in enumerate(copies)]
    for copy in copies:
        copy.start()
    for copy in copies[:2]:
        copy.wait()
    where_to = cells[0]
    row_no = lax.broadcasted_iota(jnp.int32, (px * cy, conn), 0)
    lane_no = lax.broadcasted_iota(jnp.int32, (tile, conn), 0)
    lanes = jnp.where(lane_no == where_to % tile, 1.0, 0.0).astype(jnp.bfloat16)
    rows = jnp.where(row_no == where_to // tile, index[0], 0.0)
    added = sum(nt_dot(part, lanes) for part in split3(rows))
    for copy in copies[2:]:
        copy.wait()
    for pair in range(px):
        accum_w = near_accum[pair] + added[pair * cy : (pair + 1) * cy]
        for c in range(phases):
            number = CPL + c * phases + c
            block[number, pair] = block[number, pair] + accum_w
        block[IDX, pair] = (groups[pair] + flags[4]).astype(jnp.float32)
    for number in range(FIELDS):
        one, two = sent(flags, 0, block[number, px - 1], block[number, 0])
        first[number] = one
        second[number] = two
    for place, number in enumerate(OUTER_X):
        one, two = sent(flags, 0, block[number, px - 2], block[number, 1])
        first[FIELDS + place] = one
        second[FIELDS + place] = two


def pack_narrow(flags, block, got_first, got_second, own, first, second):
    px, cy, tile = block.shape[1:]
    width = px + 2 * HX
    own_rows = rows_of(own)

    def put(number, pair, values):
        own_rows[pl.ds(number * cy * width + pair, cy, stride=width), :] = values

    for number in range(FIELDS):
        low, high = received(flags, 0, got_first[number], got_second[number])
        put(number, HX - 1, low)
        put(number, HX + px, high)
        if number in OUTER_X:
            place = FIELDS + OUTER_X.index(number)
            low, high = received(flags, 0, got_first[place], got_second[place])
        else:
            low = high = jnp.zeros((cy, tile), jnp.float32)
        put(number, 0, low)
        put(number, width - 1, high)
        for pair in range(px):
            put(number, HX + pair, block[number, pair])
    for number in range(FIELDS):
        for column in range(HY - 1):
            one, two = sent(flags, 1, own[number, cy - HY + 1 + column], own[number, column])
            first[number * (HY - 1) + column] = one
            second[number * (HY - 1) + column] = two
    for place, number in enumerate(OUTER_Y):
        one, two = sent(flags, 1, own[number, cy - HY], own[number, HY - 1])
        first[FIELDS * (HY - 1) + place] = one
        second[FIELDS * (HY - 1) + place] = two


def lane_half(shape):
    return lax.broadcasted_iota(jnp.int32, shape, len(shape) - 1) < shape[-1] // 2


def swap_half(values):
    return pltpu.roll(values, values.shape[-1] // 2, values.ndim - 1)


def east_of(values, half):
    turned = swap_half(values)
    return jnp.where(half, turned, pltpu.roll(turned, values.shape[-2] - 1, values.ndim - 2))


def west_of(values, half):
    turned = swap_half(values)
    return jnp.where(half, pltpu.roll(turned, 1, values.ndim - 2), turned)


def above(values):
    return pltpu.roll(values, values.shape[-1] - 1, values.ndim - 1)


def below(values):
    return pltpu.roll(values, 1, values.ndim - 1)


def operate(field, coeffs, column, half):
    phases = 3
    here = [field(c, column) for c in range(phases)]
    tx, ty, tz = coeffs[0, column], coeffs[1, column], coeffs[2, column]
    ty_before = coeffs[1, column - 1]
    results = []
    for c in range(phases):
        value = here[c]
        mixed = sum(coeffs[GC + c * phases + b, column] * here[b] for b in range(phases))
        inflow = tx * east_of(value, half) + west_of(tx * value, half)
        inflow = inflow + (ty * field(c, column + 1) + ty_before * field(c, column - 1))
        inflow = inflow + (tz * above(value) + below(tz * value))
        results.append(mixed - inflow)
    return results


def coarse_share(own_misfit, agg_rows, cinv, share, slots, px, cy, narrow):
    count, total = cinv.shape
    lanes = total // share.shape[0]
    width = px + 2 * HX
    agg_no = lax.broadcasted_iota(jnp.int32, (count, own_misfit.shape[-1]), 0)
    parts = [jnp.zeros(agg_no.shape, jnp.float32) for _ in range(4)]
    for column in range(cy):
        for pair in range(px):
            row = column * width + HX + pair
            here = agg_rows[pl.ds(row, 1), :]
            value = own_misfit[pl.ds(row, 1), :]
            spot = (column * px + pair) % len(parts)
            parts[spot] = parts[spot] + jnp.where(agg_no == here, value, 0.0)
    sums = jnp.sum((parts[0] + parts[1]) + (parts[2] + parts[3]), axis=1, keepdims=True)
    wide = share.shape[0]
    for i in range(wide):
        share[pl.ds(i, 1), :] = jnp.sum(cinv[:, i * lanes : (i + 1) * lanes] * sums, axis=0, keepdims=True)
    for i in range(wide):
        for place in range(3):
            row = share[pl.ds((i + place - 1) % wide, 1), :]
            for j in range(narrow):
                slots[i * narrow + j, pl.ds(place, 1), :] = row


def find_misfit(coeffs, current, misfit, own_misfit):
    columns = current.shape[1]
    cy = columns - 2 * HY
    half = lane_half(current.shape[2:])
    for column in range(1, columns - 1):
        applied = operate(lambda c, y: current[c, y], coeffs, column, half)
        for c in range(3):
            value = coeffs[GR + c, column] - applied[c]
            misfit[c, column] = value
            if c == 0 and HY <= column < HY + cy:
                own_misfit[column - HY] = value


def sweep_body(flags, coeffs, current, index, cinv, hot, cold, slots, first, second, third, fourth, px, narrow, scratch, before):
    misfit, work, hold, own_misfit, own_agg, share, update, near_slots, near_corners, sems = scratch
    cy = update.shape[1]
    owned = lax.broadcasted_iota(jnp.int32, current.shape[2:], 0) - HX
    owned = (owned >= 0) & (owned < px)
    before()
    find_misfit(coeffs, current, misfit, own_misfit)
    send = pltpu.make_async_copy(near_slots, slots.at[:, 0], sems.at[0])

    def send_shares():
        for column in range(cy):
            own_agg[column] = index[HY + column] - flags[4]
        coarse_share(rows_of(own_misfit), rows_of(own_agg), cinv, share, near_slots, px, cy, narrow)
        send.start()

    sends = []

    def send_corners():
        near = lane_half(update.shape[2:])
        for number, (x, y) in enumerate(CORNERS):
            rows = []
            for pairs, columns in CORNER_TILES:
                pair = HX + (px - pairs if x > 0 else pairs - 1)
                column = cy - columns if y > 0 else columns - 1
                tile = [update[c, column] for c in range(update.shape[0])]
                if pairs == 2:
                    turned = swap_half(tile[1])
                    tile[0] = jnp.where(near, turned, tile[0]) if x > 0 else jnp.where(near, tile[0], turned)
                    tile = [tile[0], tile[2]]
                rows += [value[pair : pair + 1] for value in tile]
            for spot, row in enumerate(rows):
                near_corners[number, spot // SLOT[1], pl.ds(spot % SLOT[1], 1), :] = row
            target = slots.at[flags[5 + number], pl.ds(1, SLOT[0] - 1)]
            sends.append(pltpu.make_async_copy(near_corners.at[number], target, sems.at[1 + number]))
        for corner in sends:
            corner.start()

    solve(flags, misfit, coeffs, hot, cold, update, first, second, third, fourth, work, hold, send_shares, send_corners)
    for column in range(cy):
        for c in range(update.shape[0]):
            here = jnp.where(owned, update[c, column], 0.0)
            current[c, HY + column] = current[c, HY + column] + here
    send.wait()
    for corner in sends:
        corner.wait()


def prepare(flags, own, got_first, got_second, cinv, hot, cold, coeffs, index, current, slots, first, second, third, fourth, field, *scratch, px, narrow):
    def before():
        assemble(flags, own, got_first, got_second, coeffs, index, current, field)

    sweep_body(flags, coeffs, current, index, cinv, hot, cold, slots, first, second, third, fourth, px, narrow, scratch, before)


def assemble(flags, own, got_first, got_second, coeffs, index, current, field):
    cy = own.shape[1]
    columns = cy + 2 * HY
    half = lane_half(own.shape[2:])
    depth = lax.broadcasted_iota(jnp.int32, own.shape[2:], 1) % (own.shape[3] // 2)
    for number in range(FIELDS):
        for column in range(cy):
            field[number, HY + column] = own[number, column]
        for column in range(HY - 1):
            low, high = received(
                flags, 1, got_first[number * (HY - 1) + column], got_second[number * (HY - 1) + column]
            )
            field[number, 1 + column] = low
            field[number, HY + cy + column] = high
    for place, number in enumerate(OUTER_Y):
        place = FIELDS * (HY - 1) + place
        low, high = received(flags, 1, got_first[place], got_second[place])
        field[number, 0] = low
        field[number, columns - 1] = high
    for column in range(columns):
        index[column] = field[IDX, column].astype(jnp.int32)
        for c in range(3):
            current[c, column] = field[CUR + c, column]
    coeffs[1, 0] = field[TY, 0]
    for column in range(1, columns - 1):
        tx, ty = field[TX, column], field[TY, column]
        tz = jnp.where(depth < own.shape[3] // 2 - 1, field[TZ, column], 0.0)
        faces = (tx + west_of(tx, half)) + (ty + field[TY, column - 1]) + (tz + below(tz))
        coeffs[0, column] = tx
        coeffs[1, column] = ty
        coeffs[2, column] = tz
        for number in range(9):
            value = field[CPL + number, column]
            if number % 4 == 0:
                value = value + faces
                coeffs[GI + number // 4, column] = 1.0 / value
            coeffs[GC + number, column] = value
        for c in range(3):
            coeffs[GR + c, column] = field[RHS + c, column]


def tile_apply(values, coeffs, tiles, column, first, last):
    scaled = [coeffs[GI + c, column] * values[c] for c in range(3)]
    stacked = jnp.concatenate(scaled, axis=0)
    width = scaled[0].shape[0]
    pair_no = lax.broadcasted_iota(jnp.int32, stacked.shape, 0) % width
    left = [jnp.where(pair_no == a + HX - 1, stacked, 0.0).astype(jnp.bfloat16) for a in range(first, last)]
    right = [tiles(a, column - 1) for a in range(first, last)]
    result = nt_dot(jnp.concatenate(left, axis=1), jnp.concatenate(right, axis=1))
    return [result[c * width : (c + 1) * width] for c in range(3)]


def solve(flags, misfit, coeffs, hot, cold, update, first, second, third, fourth, work, hold, send_shares, send_corners):
    phases, columns = work.shape[:2]
    cy = columns - 2 * HY
    boxes, inside = hot.shape[:2]
    width = work.shape[2]
    px = width - 2 * HX
    half = lane_half(work.shape[2:])
    side = cold.shape[1] // 2

    def tiles(a, b):
        if b < side:
            return cold[a, b]
        return hot[a, b - side] if b < side + inside else cold[a, b - inside]

    for c in range(phases):
        work[c, 0] = jnp.zeros(work.shape[2:], jnp.float32)
        work[c, columns - 1] = jnp.zeros(work.shape[2:], jnp.float32)

    def start(column):
        new = tile_apply([misfit[c, column] for c in range(phases)], coeffs, tiles, column, 0, boxes)
        for c in range(phases):
            work[c, column] = new[c]

    def step(source, target, shift, column, first_box, last_box):
        applied = operate(lambda c, y: source[c, y], coeffs, column, half)
        left = [misfit[c, column] - applied[c] for c in range(phases)]
        new = tile_apply(left, coeffs, tiles, column, first_box, last_box)
        for c in range(phases):
            target[c, column - shift] = source[c, column] + new[c]

    for column in range(1, columns - 1):
        start(column)
    send_shares()
    edge = 2 * (HY - 1)
    middle = range(2 + edge, columns - 2 - edge)
    for column in range(2, columns - 2):
        if column not in middle:
            step(work, hold, 0, column, 0, boxes)
    ends = [column for column in range(HY, HY + cy) if min(column - HY, HY + cy - 1 - column) < HY - 1]
    for column in ends:
        step(hold, update, HY, column, 1, boxes - 1)
    send_corners()
    for column in middle:
        step(work, hold, 0, column, 0, boxes)
    for column in range(HY, HY + cy):
        if column not in ends:
            step(hold, update, HY, column, 1, boxes - 1)
    rows = rows_of(update)
    for c in range(phases):
        for pair in range(HX):
            tail = rows[pl.ds(c * cy * width + px + pair, cy, stride=width), :]
            head = rows[pl.ds(c * cy * width + HX + pair, cy, stride=width), :]
            one, two = sent(flags, 0, tail, head)
            first[c, pair] = one
            second[c, pair] = two
        for column in range(HY):
            one, two = sent(flags, 1, update[c, cy - HY + column], update[c, column])
            third[c, column] = one
            fourth[c, column] = two


def advance(flags, current, index, got, slots_in, result):
    phases, columns, width, tile = current.shape
    cy = columns - 2 * HY
    px = width - 2 * HX
    total = [slots_in[d, 0] for d in range(min(4, slots_in.shape[0]))]
    for d in range(4, slots_in.shape[0]):
        total[d % 4] = total[d % 4] + slots_in[d, 0]
    total = sum(total[1:], total[0])
    pair_no = lax.broadcasted_iota(jnp.int32, (width, tile), 0)
    table = jnp.where(pair_no < HX, total[0:1], jnp.where(pair_no < HX + px, total[1:2], total[2:3]))
    owned = (pair_no >= HX) & (pair_no < HX + px)
    near = lane_half((width, tile))
    for column in range(columns):
        for c in range(phases):
            change = 0.0
            if not HY <= column < HY + cy:
                y = -1 if column < HY else 1
                place = column if y < 0 else column - HY - cy
                away = HY - column if y < 0 else place + 1
                change = jnp.where(owned, received(flags, 1, got[2][c, place], got[3][c, place])[(y + 1) // 2], 0.0)
                for number, (x, side) in enumerate(CORNERS):
                    for tile_no, (pairs, distance) in enumerate(CORNER_TILES):
                        if side == y and distance == away:
                            pair = HX - pairs if x < 0 else HX + px + pairs - 1
                            spot = SLOT[1] + 3 * tile_no + (c if pairs == 1 else c // 2)
                            source = slots_in.at[flags[5 + number], spot // SLOT[1], pl.ds(spot % SLOT[1], 1)]
                            row = jnp.broadcast_to(source[...], (width, tile))
                            if pairs == 2:
                                row = swap_half(row) if c == 1 else row
                                row = jnp.where(near, 0.0, row) if x < 0 else jnp.where(near, row, 0.0)
                            change = jnp.where(pair_no == pair, row, change)
            value = current[c, column] + change
            if c == 0:
                value = value + jnp.take_along_axis(table, index[column], axis=1)
            result[c, column] = value
    flat = rows_of(result)
    for c in range(phases):
        for pair in range(HX):
            low, high = received(flags, 0, got[0][c, pair], got[1][c, pair])
            for place, change in ((pair, low), (HX + px + pair, high)):
                where_to = pl.ds((c * columns + HY) * width + place, cy, stride=width)
                flat[where_to, :] = flat[where_to, :] + change


def next_sweep(flags, current, coeffs, index, got_0, got_1, got_2, got_3, slots_in, cinv, hot, cold, result, slots, first, second, third, fourth, *scratch, px, narrow):
    def start():
        advance(flags, current, index, (got_0, got_1, got_2, got_3), slots_in, result)

    sweep_body(flags, coeffs, result, index, cinv, hot, cold, slots, first, second, third, fourth, px, narrow, scratch, start)


def finish(flags, current, coeffs, index, got_0, got_1, got_2, got_3, slots_in, iterate, residual, result, misfit):
    advance(flags, current, index, (got_0, got_1, got_2, got_3), slots_in, result)
    phases, px, cy, _ = iterate.shape
    columns, width = current.shape[1:3]
    half = lane_half(current.shape[2:])
    for column in range(HY, HY + cy):
        applied = operate(lambda c, y: result[c, y], coeffs, column, half)
        for c in range(phases):
            misfit[c, column] = coeffs[GR + c, column] - applied[c]
    for source, target in ((rows_of(result), iterate), (rows_of(misfit), residual)):
        for c in range(phases):
            for pair in range(px):
                target[c, pair] = source[pl.ds((c * columns + HY) * width + HX + pair, cy, stride=width), :]


def swap(first, second, axis):
    count = lax.axis_size(axis)
    if count % 2:
        pairs = [[(i, (i + 1) % count) for i in range(count)], [((i + 1) % count, i) for i in range(count)]]
    else:
        pairs = [
            [(i, i ^ 1) for i in range(count)],
            [(i, (i + 1 if i % 2 else i - 1) % count) for i in range(count)],
        ]
    first = lax.ppermute(first, axis, pairs[0])
    second = lax.ppermute(second, axis, pairs[1])
    return first, second


def order_flags():
    flags = []
    for axis in ("wide", "narrow"):
        place = lax.axis_index(axis) % 2
        odd = lax.axis_size(axis) % 2
        flags += [0, 1] if odd else [place, place]
    flags.append(lax.axis_index("narrow") * AGG_LOC)
    for x, y in CORNERS:
        row = (lax.axis_index("wide") + x) % lax.axis_size("wide")
        flags.append(row * lax.axis_size("narrow") + (lax.axis_index("narrow") + y) % lax.axis_size("narrow"))
    return jnp.stack([jnp.asarray(flag, jnp.int32) for flag in flags])


def per_device(
    rhs,
    start,
    trans,
    accum,
    coupling,
    well_cells,
    well_index,
    agg_map,
    tile_factors,
    coarse_inverse,
):
    phases, px, cy, tile = rhs.shape
    wide, narrow = lax.axis_size("wide"), lax.axis_size("narrow")
    width, columns = px + 2 * HX, cy + 2 * HY
    f32 = jnp.float32
    flags = order_flags()
    lanes = narrow * AGG_LOC
    if min(wide, narrow) < 3 or lanes != tile:
        raise ValueError("unsupported mesh")

    boxes = tile_factors.shape
    cold = ((boxes[0], 2 * COLD) + boxes[2:], tile_factors.dtype)
    hot = ((boxes[0], boxes[1] - 2 * COLD) + boxes[2:], tile_factors.dtype)

    def tiles_after(value, outs):
        return call(fetch, outs, [pltpu.SemaphoreType.DMA((3,))], far=(0,))(flags, tile_factors, value)

    face = ((FIELDS + len(OUTER_X), cy, tile), f32)
    block, first, second = call(
        pack_wide,
        [((FIELDS, px, cy, tile), f32), face, face],
        [
            pltpu.VMEM((px, cy, tile), jnp.int32),
            pltpu.VMEM((px, cy, tile), f32),
            pltpu.VMEM(well_cells.shape, jnp.int32),
            pltpu.VMEM(well_index.shape, f32),
            pltpu.SemaphoreType.DMA((7 + phases,)),
        ],
        far=range(8),
    )(flags, trans, accum, coupling, rhs, start, agg_map, well_cells, well_index)
    first, second = swap(first, second, "wide")
    face = ((FIELDS * (HY - 1) + len(OUTER_Y), width, tile), f32)
    own, first, second = call(pack_narrow, [((FIELDS, cy, width, tile), f32), face, face])(
        flags, block, first, second
    )
    first, second = swap(first, second, "narrow")
    cold_tiles, hot_tiles = tiles_after(own, [cold, hot])

    vec = (width, tile)
    field = ((phases, columns) + vec, f32)
    inner = ((phases, columns - 1) + vec, f32)
    slot = ((wide * narrow,) + SLOT + (lanes,), f32)
    part = ((phases, cy) + vec, f32)
    face = ((phases, HX, cy, tile), f32)
    edge_face = ((phases, HY) + vec, f32)
    scratch = [
        pltpu.VMEM(*inner),
        pltpu.VMEM(*field),
        pltpu.VMEM(*field),
        pltpu.VMEM((cy,) + vec, f32),
        pltpu.VMEM((cy,) + vec, jnp.int32),
        pltpu.VMEM((wide, lanes), f32),
        pltpu.VMEM(*part),
        pltpu.VMEM((wide * narrow,) + SLOT[1:] + (lanes,), f32),
        pltpu.VMEM((len(CORNERS), SLOT[0] - 1) + SLOT[1:] + (lanes,), f32),
        pltpu.SemaphoreType.DMA((1 + len(CORNERS),)),
    ]
    faces = [face, face, edge_face, edge_face]
    coeffs, index, current, slots, *sends = call(
        functools.partial(prepare, px=px, narrow=narrow),
        [((GFIELDS, columns - 1) + vec, f32), ((columns,) + vec, jnp.int32), field, slot] + faces,
        [pltpu.VMEM((FIELDS, columns) + vec, f32)] + scratch,
        far_outs=(3,),
    )(flags, own, first, second, coarse_inverse, hot_tiles, cold_tiles)
    for sweep in range(SWEEPS):
        gathered = lax.all_to_all(slots, ("wide", "narrow"), 0, 0, tiled=True)
        got = swap(*sends[:2], "wide") + swap(*sends[2:], "narrow")
        if sweep < SWEEPS - 1:
            (cold_tiles,) = tiles_after(gathered, [cold])
        if sweep < SWEEPS - 1:
            current, slots, *sends = call(
                functools.partial(next_sweep, px=px, narrow=narrow),
                [field, slot] + faces,
                scratch,
                far_outs=(1,),
            )(flags, current, coeffs, index, *got, gathered, coarse_inverse, hot_tiles, cold_tiles)
    out = (rhs.shape, f32)
    return call(finish, [out, out], [pltpu.VMEM(*field), pltpu.VMEM(*field)])(
        flags, current, coeffs, index, *got, gathered
    )


def solution(mesh):
    return jax.shard_map(
        per_device,
        mesh=mesh,
        in_specs=(
            P(None, "wide", "narrow", None),
            P(None, "wide", "narrow", None),
            P(None, "wide", "narrow", None),
            P("wide", "narrow", None),
            P(None, None, "wide", "narrow", None),
            P("wide", "narrow", None),
            P("wide", "narrow", None),
            P("wide", "narrow", None),
            P("wide", "narrow", None, None),
            P(("wide", "narrow"), None),
        ),
        out_specs=(P(None, "wide", "narrow", None), P(None, "wide", "narrow", None)),
        check_vma=False,
    )
```

```python
import functools

import jax
import jax.numpy as jnp
from jax import lax
from jax.experimental import pallas as pl
from jax.experimental.pallas import tpu as pltpu
from jax.sharding import PartitionSpec as P

AGG_LOC = 32
SWEEPS = 3
HX = 2
HY = 3

TX, TY, TZ, CPL, RHS, CUR, IDX, FIELDS = 0, 1, 2, 3, 12, 15, 18, 19
OUTER_X = (TX, CUR, CUR + 1, CUR + 2, IDX)
OUTER_Y = (TY, CUR, CUR + 1, CUR + 2, IDX)
NEXT_Y = (TX,) + OUTER_Y
NEXT_X = OUTER_X
CORNERS = ((-1, -1), (-1, 1), (1, -1), (1, 1))
CORNER_TILES = ((1, 1), (1, 2), (2, 1))
COLD = 2
SLOT = (3, 4)
GC, GI, GR, GFIELDS = 3, 12, 15, 18

PARAMS = pltpu.CompilerParams(vmem_limit_bytes=16 * 1024 * 1024)


HBM = pl.BlockSpec(memory_space=pltpu.HBM)
VMEM = pl.BlockSpec(memory_space=pltpu.VMEM)


def call(body, outs, scratch=(), far=(), far_outs=()):
    def run(flags, *args):
        specs = [pl.BlockSpec(memory_space=pltpu.SMEM)]
        specs += [HBM if number in far else VMEM for number in range(len(args))]
        args = [
            pltpu.with_memory_space_constraint(arg, pltpu.HBM) if number in far else arg
            for number, arg in enumerate(args)
        ]
        return pl.pallas_call(
            body,
            out_shape=tuple(
                (pltpu.HBM if number in far_outs else jax.ShapeDtypeStruct)(*out) for number, out in enumerate(outs)
            ),
            in_specs=specs,
            out_specs=tuple(HBM if number in far_outs else VMEM for number in range(len(outs))),
            scratch_shapes=list(scratch),
            compiler_params=PARAMS,
        )(flags, *args)

    return run


def rows_of(ref):
    size = 1
    for length in ref.shape[:-1]:
        size *= length
    return ref.reshape(size, ref.shape[-1])


def sent(flags, axis, tail, head):
    low_first = flags[2 * axis] == 0
    return jnp.where(low_first, tail, head), jnp.where(low_first, head, tail)


def received(flags, axis, first, second):
    swapped = flags[2 * axis + 1] == 0
    return jnp.where(swapped, second, first), jnp.where(swapped, first, second)


def split3(values):
    high = values.astype(jnp.bfloat16)
    rest = values - high.astype(jnp.float32)
    middle = rest.astype(jnp.bfloat16)
    low = (rest - middle.astype(jnp.float32)).astype(jnp.bfloat16)
    return high, middle, low


def nt_dot(left, right):
    return lax.dot_general(left, right, (((1,), (1,)), ((), ())), preferred_element_type=jnp.float32)


def fetch(flags, factors, after, *refs):
    *near, sems = refs
    cold = near[0]
    side = cold.shape[1] // 2
    inside = factors.shape[1] - 2 * side
    copies = [
        (factors.at[:, pl.ds(0, side)], cold.at[:, pl.ds(0, side)]),
        (factors.at[:, pl.ds(side + inside, side)], cold.at[:, pl.ds(side, side)]),
    ]
    copies += [(factors.at[:, pl.ds(side, inside)], hot) for hot in near[1:]]
    copies = [pltpu.make_async_copy(source, target, sems.at[k]) for k, (source, target) in enumerate(copies)]
    for copy in copies:
        copy.start()
    for copy in copies:
        copy.wait()


def pack_wide(flags, trans, accum, coupling, rhs, start, agg, far_cells, far_index, block, first, second, groups, near_accum, cells, index, sems):
    phases, px, cy, tile = rhs.shape
    conn = cells.shape[-1]
    copies = [
        (far_cells, cells),
        (far_index, index),
        (accum, near_accum),
        (agg, groups),
        (trans, block.at[pl.ds(TX, 3)]),
        (rhs, block.at[pl.ds(RHS, phases)]),
        (start, block.at[pl.ds(CUR, phases)]),
    ]
    copies += [(coupling.at[c], block.at[pl.ds(CPL + c * phases, phases)]) for c in range(phases)]
    copies = [pltpu.make_async_copy(source, target, sems.at[k]) for k, (source, target) in enumerate(copies)]
    for copy in copies:
        copy.start()
    for copy in copies[:2]:
        copy.wait()
    where_to = cells[0]
    row_no = lax.broadcasted_iota(jnp.int32, (px * cy, conn), 0)
    lane_no = lax.broadcasted_iota(jnp.int32, (tile, conn), 0)
    lanes = jnp.where(lane_no == where_to % tile, 1.0, 0.0).astype(jnp.bfloat16)
    rows = jnp.where(row_no == where_to // tile, index[0], 0.0)
    added = sum(nt_dot(part, lanes) for part in split3(rows))
    for copy in copies[2:]:
        copy.wait()
    for pair in range(px):
        accum_w = near_accum[pair] + added[pair * cy : (pair + 1) * cy]
        for c in range(phases):
            number = CPL + c * phases + c
            block[number, pair] = block[number, pair] + accum_w
        block[IDX, pair] = (groups[pair] + flags[4]).astype(jnp.float32)
    for number in range(FIELDS):
        one, two = sent(flags, 0, block[number, px - 1], block[number, 0])
        first[number] = one
        second[number] = two
    for place, number in enumerate(OUTER_X):
        one, two = sent(flags, 0, block[number, px - 2], block[number, 1])
        first[FIELDS + place] = one
        second[FIELDS + place] = two


def narrow_rows(px):
    return -(-(FIELDS * (HY - 1) + len(OUTER_Y)) * px // 8) * 8


CORNER_ROWS = -(-2 * (FIELDS + len(NEXT_Y) + len(NEXT_X)) // 8) * 8


def pack_narrow(flags, block, first, second):
    px, cy, _ = block.shape[1:]
    rows = rows_of(block)

    def put(place, number, tail, head):
        sides = [rows[pl.ds(number * px * cy + column, px, stride=cy), :] for column in (tail, head)]
        one, two = sent(flags, 1, *sides)
        first[pl.ds(place * px, px), :] = one
        second[pl.ds(place * px, px), :] = two

    for number in range(FIELDS):
        for column in range(HY - 1):
            put(number * (HY - 1) + column, number, cy - HY + 1 + column, column)
    for place, number in enumerate(OUTER_Y):
        put(FIELDS * (HY - 1) + place, number, cy - HY, HY - 1)


def corner_fields():
    rows = [(number, number, 1, 1) for number in range(FIELDS)]
    rows += [(number, number, 1, 2) for number in NEXT_Y]
    return rows + [(number, FIELDS + place, 2, 1) for place, number in enumerate(NEXT_X)]


def pack_corners(flags, got_first, got_second, first, second):
    cy = got_first.shape[1]
    row = 0
    for side in range(2):
        for _, place, _, distance in corner_fields():
            sides = []
            for column in (cy - distance, distance - 1):
                pair = [got[place, pl.ds(column, 1), :] for got in (got_first, got_second)]
                sides.append(received(flags, 0, *pair)[side])
            one, two = sent(flags, 1, *sides)
            first[pl.ds(row, 1), :] = one
            second[pl.ds(row, 1), :] = two
            row += 1


def spread(flags, block, wide_first, wide_second, narrow_first, narrow_second, corner_first, corner_second, field):
    px, cy, tile = block.shape[1:]
    columns, width = field.shape[1:3]
    rows = rows_of(field)
    empty = jnp.zeros((width, tile), jnp.float32)

    def put(number, pair, values):
        rows[pl.ds((number * columns + HY) * width + pair, cy, stride=width), :] = values

    for number in range(FIELDS):
        for column in range(HY):
            field[number, column] = empty
            field[number, HY + cy + column] = empty
        for pair in range(px):
            put(number, HX + pair, block[number, pair])
        low, high = received(flags, 0, wide_first[number], wide_second[number])
        put(number, HX - 1, low)
        put(number, HX + px, high)
        if number in OUTER_X:
            place = FIELDS + OUTER_X.index(number)
            low, high = received(flags, 0, wide_first[place], wide_second[place])
        else:
            low = high = jnp.zeros((cy, tile), jnp.float32)
        put(number, 0, low)
        put(number, width - 1, high)
    places = [(number, 1 + column, HY + cy + column) for number in range(FIELDS) for column in range(HY - 1)]
    places += [(number, 0, columns - 1) for number in OUTER_Y]
    for place, (number, before, after) in enumerate(places):
        some = pl.ds(place * px, px)
        low, high = received(flags, 1, narrow_first[some, :], narrow_second[some, :])
        field[number, before, pl.ds(HX, px), :] = low
        field[number, after, pl.ds(HX, px), :] = high
    row = 0
    for side in range(2):
        for number, _, pairs, distance in corner_fields():
            pair = HX - pairs if side == 0 else HX + px + pairs - 1
            some = pl.ds(row, 1)
            low, high = received(flags, 1, corner_first[some, :], corner_second[some, :])
            field[number, HY - distance, pl.ds(pair, 1), :] = low
            field[number, HY + cy + distance - 1, pl.ds(pair, 1), :] = high
            row += 1


def lane_half(shape):
    return lax.broadcasted_iota(jnp.int32, shape, len(shape) - 1) < shape[-1] // 2


def swap_half(values):
    return pltpu.roll(values, values.shape[-1] // 2, values.ndim - 1)


def east_of(values, half):
    turned = swap_half(values)
    return jnp.where(half, turned, pltpu.roll(turned, values.shape[-2] - 1, values.ndim - 2))


def west_of(values, half):
    turned = swap_half(values)
    return jnp.where(half, pltpu.roll(turned, 1, values.ndim - 2), turned)


def above(values):
    return pltpu.roll(values, values.shape[-1] - 1, values.ndim - 1)


def below(values):
    return pltpu.roll(values, 1, values.ndim - 1)


def operate(field, coeffs, column, half):
    phases = 3
    here = [field(c, column) for c in range(phases)]
    tx, ty, tz = coeffs[0, column], coeffs[1, column], coeffs[2, column]
    ty_before = coeffs[1, column - 1]
    results = []
    for c in range(phases):
        value = here[c]
        mixed = sum(coeffs[GC + c * phases + b, column] * here[b] for b in range(phases))
        inflow = tx * east_of(value, half) + west_of(tx * value, half)
        inflow = inflow + (ty * field(c, column + 1) + ty_before * field(c, column - 1))
        inflow = inflow + (tz * above(value) + below(tz * value))
        results.append(mixed - inflow)
    return results


def coarse_share(own_misfit, agg_rows, cinv, share, slots, px, cy, narrow):
    count, total = cinv.shape
    lanes = total // share.shape[0]
    width = px + 2 * HX
    agg_no = lax.broadcasted_iota(jnp.int32, (count, own_misfit.shape[-1]), 0)
    parts = [jnp.zeros(agg_no.shape, jnp.float32) for _ in range(4)]
    for column in range(cy):
        for pair in range(px):
            row = column * width + HX + pair
            here = agg_rows[pl.ds(row, 1), :]
            value = own_misfit[pl.ds(row, 1), :]
            spot = (column * px + pair) % len(parts)
            parts[spot] = parts[spot] + jnp.where(agg_no == here, value, 0.0)
    sums = jnp.sum((parts[0] + parts[1]) + (parts[2] + parts[3]), axis=1, keepdims=True)
    wide = share.shape[0]
    for i in range(wide):
        share[pl.ds(i, 1), :] = jnp.sum(cinv[:, i * lanes : (i + 1) * lanes] * sums, axis=0, keepdims=True)
    for i in range(wide):
        for place in range(3):
            row = share[pl.ds((i + place - 1) % wide, 1), :]
            for j in range(narrow):
                slots[i * narrow + j, pl.ds(place, 1), :] = row


def find_misfit(coeffs, current, misfit, own_misfit):
    columns = current.shape[1]
    cy = columns - 2 * HY
    half = lane_half(current.shape[2:])
    for column in range(1, columns - 1):
        applied = operate(lambda c, y: current[c, y], coeffs, column, half)
        for c in range(3):
            value = coeffs[GR + c, column] - applied[c]
            misfit[c, column] = value
            if c == 0 and HY <= column < HY + cy:
                own_misfit[column - HY] = value


def sweep_body(flags, coeffs, current, index, cinv, hot, cold, slots, first, second, third, fourth, px, narrow, scratch, before):
    misfit, work, hold, own_misfit, own_agg, share, update, near_slots, near_corners, sems = scratch
    cy = update.shape[1]
    owned = lax.broadcasted_iota(jnp.int32, current.shape[2:], 0) - HX
    owned = (owned >= 0) & (owned < px)
    before()
    find_misfit(coeffs, current, misfit, own_misfit)
    send = pltpu.make_async_copy(near_slots, slots.at[:, 0], sems.at[0])

    def send_shares():
        for column in range(cy):
            own_agg[column] = index[HY + column] - flags[4]
        coarse_share(rows_of(own_misfit), rows_of(own_agg), cinv, share, near_slots, px, cy, narrow)
        send.start()

    sends = []

    def send_corners():
        near = lane_half(update.shape[2:])
        for number, (x, y) in enumerate(CORNERS):
            rows = []
            for pairs, columns in CORNER_TILES:
                pair = HX + (px - pairs if x > 0 else pairs - 1)
                column = cy - columns if y > 0 else columns - 1
                tile = [update[c, column] for c in range(update.shape[0])]
                if pairs == 2:
                    turned = swap_half(tile[1])
                    tile[0] = jnp.where(near, turned, tile[0]) if x > 0 else jnp.where(near, tile[0], turned)
                    tile = [tile[0], tile[2]]
                rows += [value[pair : pair + 1] for value in tile]
            for spot, row in enumerate(rows):
                near_corners[number, spot // SLOT[1], pl.ds(spot % SLOT[1], 1), :] = row
            target = slots.at[flags[5 + number], pl.ds(1, SLOT[0] - 1)]
            sends.append(pltpu.make_async_copy(near_corners.at[number], target, sems.at[1 + number]))
        for corner in sends:
            corner.start()

    solve(flags, misfit, coeffs, hot, cold, update, first, second, third, fourth, work, hold, send_shares, send_corners)
    for column in range(cy):
        for c in range(update.shape[0]):
            here = jnp.where(owned, update[c, column], 0.0)
            current[c, HY + column] = current[c, HY + column] + here
    send.wait()
    for corner in sends:
        corner.wait()


def prepare(flags, block, wide_first, wide_second, narrow_first, narrow_second, corner_first, corner_second, cinv, hot, cold, coeffs, index, current, slots, first, second, third, fourth, field, *scratch, px, narrow):
    def before():
        got = (wide_first, wide_second, narrow_first, narrow_second, corner_first, corner_second)
        spread(flags, block, *got, field)
        assemble(coeffs, index, current, field)

    sweep_body(flags, coeffs, current, index, cinv, hot, cold, slots, first, second, third, fourth, px, narrow, scratch, before)


def assemble(coeffs, index, current, field):
    columns, width, tile = field.shape[1:]
    half = lane_half((width, tile))
    depth = lax.broadcasted_iota(jnp.int32, (width, tile), 1) % (tile // 2)
    for column in range(columns):
        index[column] = field[IDX, column].astype(jnp.int32)
        for c in range(3):
            current[c, column] = field[CUR + c, column]
    coeffs[1, 0] = field[TY, 0]
    for column in range(1, columns - 1):
        tx, ty = field[TX, column], field[TY, column]
        tz = jnp.where(depth < tile // 2 - 1, field[TZ, column], 0.0)
        faces = (tx + west_of(tx, half)) + (ty + field[TY, column - 1]) + (tz + below(tz))
        coeffs[0, column] = tx
        coeffs[1, column] = ty
        coeffs[2, column] = tz
        for number in range(9):
            value = field[CPL + number, column]
            if number % 4 == 0:
                value = value + faces
                coeffs[GI + number // 4, column] = 1.0 / value
            coeffs[GC + number, column] = value
        for c in range(3):
            coeffs[GR + c, column] = field[RHS + c, column]


def tile_apply(values, coeffs, tiles, column, first, last):
    scaled = [coeffs[GI + c, column] * values[c] for c in range(3)]
    stacked = jnp.concatenate(scaled, axis=0)
    width = scaled[0].shape[0]
    pair_no = lax.broadcasted_iota(jnp.int32, stacked.shape, 0) % width
    left = [jnp.where(pair_no == a + HX - 1, stacked, 0.0).astype(jnp.bfloat16) for a in range(first, last)]
    right = [tiles(a, column - 1) for a in range(first, last)]
    result = nt_dot(jnp.concatenate(left, axis=1), jnp.concatenate(right, axis=1))
    return [result[c * width : (c + 1) * width] for c in range(3)]


def solve(flags, misfit, coeffs, hot, cold, update, first, second, third, fourth, work, hold, send_shares, send_corners):
    phases, columns = work.shape[:2]
    cy = columns - 2 * HY
    boxes, inside = hot.shape[:2]
    width = work.shape[2]
    px = width - 2 * HX
    half = lane_half(work.shape[2:])
    side = cold.shape[1] // 2

    def tiles(a, b):
        if b < side:
            return cold[a, b]
        return hot[a, b - side] if b < side + inside else cold[a, b - inside]

    for c in range(phases):
        work[c, 0] = jnp.zeros(work.shape[2:], jnp.float32)
        work[c, columns - 1] = jnp.zeros(work.shape[2:], jnp.float32)

    def start(column):
        new = tile_apply([misfit[c, column] for c in range(phases)], coeffs, tiles, column, 0, boxes)
        for c in range(phases):
            work[c, column] = new[c]

    def step(source, target, shift, column, first_box, last_box):
        applied = operate(lambda c, y: source[c, y], coeffs, column, half)
        left = [misfit[c, column] - applied[c] for c in range(phases)]
        new = tile_apply(left, coeffs, tiles, column, first_box, last_box)
        for c in range(phases):
            target[c, column - shift] = source[c, column] + new[c]

    for column in range(1, columns - 1):
        start(column)
    send_shares()
    edge = 2 * (HY - 1)
    middle = range(2 + edge, columns - 2 - edge)
    for column in range(2, columns - 2):
        if column not in middle:
            step(work, hold, 0, column, 0, boxes)
    ends = [column for column in range(HY, HY + cy) if min(column - HY, HY + cy - 1 - column) < HY - 1]
    for column in ends:
        step(hold, update, HY, column, 1, boxes - 1)
    send_corners()
    for column in middle:
        step(work, hold, 0, column, 0, boxes)
    for column in range(HY, HY + cy):
        if column not in ends:
            step(hold, update, HY, column, 1, boxes - 1)
    rows = rows_of(update)
    for c in range(phases):
        for pair in range(HX):
            tail = rows[pl.ds(c * cy * width + px + pair, cy, stride=width), :]
            head = rows[pl.ds(c * cy * width + HX + pair, cy, stride=width), :]
            one, two = sent(flags, 0, tail, head)
            first[c, pair] = one
            second[c, pair] = two
        for column in range(HY):
            one, two = sent(flags, 1, update[c, cy - HY + column], update[c, column])
            third[c, column] = one
            fourth[c, column] = two


def advance(flags, current, index, got, slots_in, result):
    phases, columns, width, tile = current.shape
    cy = columns - 2 * HY
    px = width - 2 * HX
    total = [slots_in[d, 0] for d in range(min(4, slots_in.shape[0]))]
    for d in range(4, slots_in.shape[0]):
        total[d % 4] = total[d % 4] + slots_in[d, 0]
    total = sum(total[1:], total[0])
    pair_no = lax.broadcasted_iota(jnp.int32, (width, tile), 0)
    table = jnp.where(pair_no < HX, total[0:1], jnp.where(pair_no < HX + px, total[1:2], total[2:3]))
    owned = (pair_no >= HX) & (pair_no < HX + px)
    near = lane_half((width, tile))
    for column in range(columns):
        for c in range(phases):
            change = 0.0
            if not HY <= column < HY + cy:
                y = -1 if column < HY else 1
                place = column if y < 0 else column - HY - cy
                away = HY - column if y < 0 else place + 1
                change = jnp.where(owned, received(flags, 1, got[2][c, place], got[3][c, place])[(y + 1) // 2], 0.0)
                for number, (x, side) in enumerate(CORNERS):
                    for tile_no, (pairs, distance) in enumerate(CORNER_TILES):
                        if side == y and distance == away:
                            pair = HX - pairs if x < 0 else HX + px + pairs - 1
                            spot = SLOT[1] + 3 * tile_no + (c if pairs == 1 else c // 2)
                            source = slots_in.at[flags[5 + number], spot // SLOT[1], pl.ds(spot % SLOT[1], 1)]
                            row = jnp.broadcast_to(source[...], (width, tile))
                            if pairs == 2:
                                row = swap_half(row) if c == 1 else row
                                row = jnp.where(near, 0.0, row) if x < 0 else jnp.where(near, row, 0.0)
                            change = jnp.where(pair_no == pair, row, change)
            value = current[c, column] + change
            if c == 0:
                value = value + jnp.take_along_axis(table, index[column], axis=1)
            result[c, column] = value
    flat = rows_of(result)
    for c in range(phases):
        for pair in range(HX):
            low, high = received(flags, 0, got[0][c, pair], got[1][c, pair])
            for place, change in ((pair, low), (HX + px + pair, high)):
                where_to = pl.ds((c * columns + HY) * width + place, cy, stride=width)
                flat[where_to, :] = flat[where_to, :] + change


def next_sweep(flags, current, coeffs, index, got_0, got_1, got_2, got_3, slots_in, cinv, hot, cold, result, slots, first, second, third, fourth, *scratch, px, narrow):
    def start():
        advance(flags, current, index, (got_0, got_1, got_2, got_3), slots_in, result)

    sweep_body(flags, coeffs, result, index, cinv, hot, cold, slots, first, second, third, fourth, px, narrow, scratch, start)


def finish(flags, current, coeffs, index, got_0, got_1, got_2, got_3, slots_in, iterate, residual, result, misfit):
    advance(flags, current, index, (got_0, got_1, got_2, got_3), slots_in, result)
    phases, px, cy, _ = iterate.shape
    columns, width = current.shape[1:3]
    half = lane_half(current.shape[2:])
    for column in range(HY, HY + cy):
        applied = operate(lambda c, y: result[c, y], coeffs, column, half)
        for c in range(phases):
            misfit[c, column] = coeffs[GR + c, column] - applied[c]
    for source, target in ((rows_of(result), iterate), (rows_of(misfit), residual)):
        for c in range(phases):
            for pair in range(px):
                target[c, pair] = source[pl.ds((c * columns + HY) * width + HX + pair, cy, stride=width), :]


def swap(first, second, axis):
    count = lax.axis_size(axis)
    if count % 2:
        pairs = [[(i, (i + 1) % count) for i in range(count)], [((i + 1) % count, i) for i in range(count)]]
    else:
        pairs = [
            [(i, i ^ 1) for i in range(count)],
            [(i, (i + 1 if i % 2 else i - 1) % count) for i in range(count)],
        ]
    first = lax.ppermute(first, axis, pairs[0])
    second = lax.ppermute(second, axis, pairs[1])
    return first, second


def order_flags():
    flags = []
    for axis in ("wide", "narrow"):
        place = lax.axis_index(axis) % 2
        odd = lax.axis_size(axis) % 2
        flags += [0, 1] if odd else [place, place]
    flags.append(lax.axis_index("narrow") * AGG_LOC)
    for x, y in CORNERS:
        row = (lax.axis_index("wide") + x) % lax.axis_size("wide")
        flags.append(row * lax.axis_size("narrow") + (lax.axis_index("narrow") + y) % lax.axis_size("narrow"))
    return jnp.stack([jnp.asarray(flag, jnp.int32) for flag in flags])


def per_device(
    rhs,
    start,
    trans,
    accum,
    coupling,
    well_cells,
    well_index,
    agg_map,
    tile_factors,
    coarse_inverse,
):
    phases, px, cy, tile = rhs.shape
    wide, narrow = lax.axis_size("wide"), lax.axis_size("narrow")
    width, columns = px + 2 * HX, cy + 2 * HY
    f32 = jnp.float32
    flags = order_flags()
    lanes = narrow * AGG_LOC
    if min(wide, narrow) < 3 or lanes != tile:
        raise ValueError("unsupported mesh")

    boxes = tile_factors.shape
    cold = ((boxes[0], 2 * COLD) + boxes[2:], tile_factors.dtype)
    hot = ((boxes[0], boxes[1] - 2 * COLD) + boxes[2:], tile_factors.dtype)

    def tiles_after(value, outs):
        return call(fetch, outs, [pltpu.SemaphoreType.DMA((3,))], far=(0,))(flags, tile_factors, value)

    face = ((FIELDS + len(OUTER_X), cy, tile), f32)
    block, first, second = call(
        pack_wide,
        [((FIELDS, px, cy, tile), f32), face, face],
        [
            pltpu.VMEM((px, cy, tile), jnp.int32),
            pltpu.VMEM((px, cy, tile), f32),
            pltpu.VMEM(well_cells.shape, jnp.int32),
            pltpu.VMEM(well_index.shape, f32),
            pltpu.SemaphoreType.DMA((7 + phases,)),
        ],
        far=range(8),
    )(flags, trans, accum, coupling, rhs, start, agg_map, well_cells, well_index)
    got = swap(first, second, "wide")
    face = ((narrow_rows(px), tile), f32)
    got += swap(*call(pack_narrow, [face, face])(flags, block), "narrow")
    cold_tiles, hot_tiles = tiles_after(block, [cold, hot])
    face = ((CORNER_ROWS, tile), f32)
    got += swap(*call(pack_corners, [face, face])(flags, *got[:2]), "narrow")

    vec = (width, tile)
    field = ((phases, columns) + vec, f32)
    inner = ((phases, columns - 1) + vec, f32)
    slot = ((wide * narrow,) + SLOT + (lanes,), f32)
    part = ((phases, cy) + vec, f32)
    face = ((phases, HX, cy, tile), f32)
    edge_face = ((phases, HY) + vec, f32)
    scratch = [
        pltpu.VMEM(*inner),
        pltpu.VMEM(*field),
        pltpu.VMEM(*field),
        pltpu.VMEM((cy,) + vec, f32),
        pltpu.VMEM((cy,) + vec, jnp.int32),
        pltpu.VMEM((wide, lanes), f32),
        pltpu.VMEM(*part),
        pltpu.VMEM((wide * narrow,) + SLOT[1:] + (lanes,), f32),
        pltpu.VMEM((len(CORNERS), SLOT[0] - 1) + SLOT[1:] + (lanes,), f32),
        pltpu.SemaphoreType.DMA((1 + len(CORNERS),)),
    ]
    faces = [face, face, edge_face, edge_face]
    coeffs, index, current, slots, *sends = call(
        functools.partial(prepare, px=px, narrow=narrow),
        [((GFIELDS, columns - 1) + vec, f32), ((columns,) + vec, jnp.int32), field, slot] + faces,
        [pltpu.VMEM((FIELDS, columns) + vec, f32)] + scratch,
        far_outs=(3,),
    )(flags, block, *got, coarse_inverse, hot_tiles, cold_tiles)
    for sweep in range(SWEEPS):
        gathered = lax.all_to_all(slots, ("wide", "narrow"), 0, 0, tiled=True)
        got = swap(*sends[:2], "wide") + swap(*sends[2:], "narrow")
        if sweep < SWEEPS - 1:
            (cold_tiles,) = tiles_after(gathered, [cold])
        if sweep < SWEEPS - 1:
            current, slots, *sends = call(
                functools.partial(next_sweep, px=px, narrow=narrow),
                [field, slot] + faces,
                scratch,
                far_outs=(1,),
            )(flags, current, coeffs, index, *got, gathered, coarse_inverse, hot_tiles, cold_tiles)
    out = (rhs.shape, f32)
    return call(finish, [out, out], [pltpu.VMEM(*field), pltpu.VMEM(*field)])(
        flags, current, coeffs, index, *got, gathered
    )


def solution(mesh):
    return jax.shard_map(
        per_device,
        mesh=mesh,
        in_specs=(
            P(None, "wide", "narrow", None),
            P(None, "wide", "narrow", None),
            P(None, "wide", "narrow", None),
            P("wide", "narrow", None),
            P(None, None, "wide", "narrow", None),
            P("wide", "narrow", None),
            P("wide", "narrow", None),
            P("wide", "narrow", None),
            P("wide", "narrow", None, None),
            P(("wide", "narrow"), None),
        ),
        out_specs=(P(None, "wide", "narrow", None), P(None, "wide", "narrow", None)),
        check_vma=False,
    )
```

```python
import functools

import jax
import jax.numpy as jnp
from jax import lax
from jax.experimental import pallas as pl
from jax.experimental.pallas import tpu as pltpu
from jax.sharding import PartitionSpec as P

AGG_LOC = 32
SWEEPS = 3
HX = 2
HY = 3

TX, TY, TZ, CPL, RHS, CUR, IDX, FIELDS = 0, 1, 2, 3, 12, 15, 18, 19
OUTER_X = (TX, CUR, CUR + 1, CUR + 2, IDX)
OUTER_Y = (TY, CUR, CUR + 1, CUR + 2, IDX)
NEXT_Y = (TX,) + OUTER_Y
NEXT_X = OUTER_X
CORNERS = ((-1, -1), (-1, 1), (1, -1), (1, 1))
CORNER_TILES = ((1, 1), (1, 2), (2, 1))
COLD = 2
SLOT = (3, 4)
GC, GI, GR, GFIELDS = 3, 12, 15, 18

PARAMS = pltpu.CompilerParams(vmem_limit_bytes=16 * 1024 * 1024)


HBM = pl.BlockSpec(memory_space=pltpu.HBM)
VMEM = pl.BlockSpec(memory_space=pltpu.VMEM)


def call(body, outs, scratch=(), far=(), far_outs=()):
    def run(flags, *args):
        specs = [pl.BlockSpec(memory_space=pltpu.SMEM)]
        specs += [HBM if number in far else VMEM for number in range(len(args))]
        args = [
            pltpu.with_memory_space_constraint(arg, pltpu.HBM) if number in far else arg
            for number, arg in enumerate(args)
        ]
        return pl.pallas_call(
            body,
            out_shape=tuple(
                (pltpu.HBM if number in far_outs else jax.ShapeDtypeStruct)(*out) for number, out in enumerate(outs)
            ),
            in_specs=specs,
            out_specs=tuple(HBM if number in far_outs else VMEM for number in range(len(outs))),
            scratch_shapes=list(scratch),
            compiler_params=PARAMS,
        )(flags, *args)

    return run


def rows_of(ref):
    size = 1
    for length in ref.shape[:-1]:
        size *= length
    return ref.reshape(size, ref.shape[-1])


def sent(flags, axis, tail, head):
    low_first = flags[2 * axis] == 0
    return jnp.where(low_first, tail, head), jnp.where(low_first, head, tail)


def received(flags, axis, first, second):
    swapped = flags[2 * axis + 1] == 0
    return jnp.where(swapped, second, first), jnp.where(swapped, first, second)


def split3(values):
    high = values.astype(jnp.bfloat16)
    rest = values - high.astype(jnp.float32)
    middle = rest.astype(jnp.bfloat16)
    low = (rest - middle.astype(jnp.float32)).astype(jnp.bfloat16)
    return high, middle, low


def nt_dot(left, right):
    return lax.dot_general(left, right, (((1,), (1,)), ((), ())), preferred_element_type=jnp.float32)


def turn(flags, factors, after, cold, hot, kept, raw, sems):
    boxes, count, tile, _ = factors.shape
    side = cold.shape[0] // 2
    inside = hot.shape[0]
    order = sorted(range(count // 2), key=lambda group: side <= group < side + inside)
    loads = {}
    for group in order:
        some = pl.ds(2 * group, 2)
        loads[group] = pltpu.make_async_copy(factors.at[:, some], raw.at[:, some], sems.at[group])
        loads[group].start()
    save = pltpu.make_async_copy(cold, kept, sems.at[count // 2])
    row_no = lax.broadcasted_iota(jnp.int32, (tile, tile), 0)
    unit = jnp.where(row_no == lax.broadcasted_iota(jnp.int32, (tile, tile), 1), 1.0, 0.0).astype(factors.dtype)
    for number, group in enumerate(order):
        if number == 2 * side:
            save.start()
        loads[group].wait()
        if group < side:
            target = cold.at[group]
        elif group < side + inside:
            target = hot.at[group - side]
        else:
            target = cold.at[group - inside]
        for place in range(2):
            stacked = jnp.concatenate([raw[a, 2 * group + place] for a in range(boxes)], axis=0)
            turned = nt_dot(unit, stacked).astype(factors.dtype)
            for a in range(boxes):
                spot = (pl.ds(a * tile, tile), pl.ds(place * tile, tile))
                target[spot] = turned[:, a * tile : (a + 1) * tile]
    save.wait()


def fetch(flags, kept, after, cold, sems):
    rows = cold.shape[1] // (sems.shape[0] // cold.shape[0])
    loads = []
    for number in range(sems.shape[0]):
        spot = (number % cold.shape[0], pl.ds(number // cold.shape[0] * rows, rows))
        loads.append(pltpu.make_async_copy(kept.at[spot], cold.at[spot], sems.at[number]))
    for load in loads:
        load.start()
    for load in loads:
        load.wait()


def pack_wide(flags, trans, accum, coupling, rhs, start, agg, far_cells, far_index, block, first, second, groups, near_accum, cells, index, sems):
    phases, px, cy, tile = rhs.shape
    conn = cells.shape[-1]
    copies = [
        (far_cells, cells),
        (far_index, index),
        (accum, near_accum),
        (agg, groups),
        (trans, block.at[pl.ds(TX, 3)]),
        (rhs, block.at[pl.ds(RHS, phases)]),
        (start, block.at[pl.ds(CUR, phases)]),
    ]
    copies += [(coupling.at[c], block.at[pl.ds(CPL + c * phases, phases)]) for c in range(phases)]
    copies = [pltpu.make_async_copy(source, target, sems.at[k]) for k, (source, target) in enumerate(copies)]
    for copy in copies:
        copy.start()
    for copy in copies[:2]:
        copy.wait()
    where_to = cells[0]
    row_no = lax.broadcasted_iota(jnp.int32, (px * cy, conn), 0)
    lane_no = lax.broadcasted_iota(jnp.int32, (tile, conn), 0)
    lanes = jnp.where(lane_no == where_to % tile, 1.0, 0.0).astype(jnp.bfloat16)
    rows = jnp.where(row_no == where_to // tile, index[0], 0.0)
    added = sum(nt_dot(part, lanes) for part in split3(rows))
    for copy in copies[2:]:
        copy.wait()
    for pair in range(px):
        accum_w = near_accum[pair] + added[pair * cy : (pair + 1) * cy]
        for c in range(phases):
            number = CPL + c * phases + c
            block[number, pair] = block[number, pair] + accum_w
        block[IDX, pair] = (groups[pair] + flags[4]).astype(jnp.float32)
    for number in range(FIELDS):
        one, two = sent(flags, 0, block[number, px - 1], block[number, 0])
        first[number] = one
        second[number] = two
    for place, number in enumerate(OUTER_X):
        one, two = sent(flags, 0, block[number, px - 2], block[number, 1])
        first[FIELDS + place] = one
        second[FIELDS + place] = two


def narrow_rows(px):
    return -(-(FIELDS * (HY - 1) + len(OUTER_Y)) * px // 8) * 8


CORNER_ROWS = -(-2 * (FIELDS + len(NEXT_Y) + len(NEXT_X)) // 8) * 8


def pack_narrow(flags, block, first, second):
    px, cy, _ = block.shape[1:]
    rows = rows_of(block)

    def put(place, number, tail, head):
        sides = [rows[pl.ds(number * px * cy + column, px, stride=cy), :] for column in (tail, head)]
        one, two = sent(flags, 1, *sides)
        first[pl.ds(place * px, px), :] = one
        second[pl.ds(place * px, px), :] = two

    for number in range(FIELDS):
        for column in range(HY - 1):
            put(number * (HY - 1) + column, number, cy - HY + 1 + column, column)
    for place, number in enumerate(OUTER_Y):
        put(FIELDS * (HY - 1) + place, number, cy - HY, HY - 1)


def corner_fields():
    rows = [(number, number, 1, 1) for number in range(FIELDS)]
    rows += [(number, number, 1, 2) for number in NEXT_Y]
    return rows + [(number, FIELDS + place, 2, 1) for place, number in enumerate(NEXT_X)]


def pack_corners(flags, got_first, got_second, first, second):
    cy = got_first.shape[1]
    row = 0
    for side in range(2):
        for _, place, _, distance in corner_fields():
            sides = []
            for column in (cy - distance, distance - 1):
                pair = [got[place, pl.ds(column, 1), :] for got in (got_first, got_second)]
                sides.append(received(flags, 0, *pair)[side])
            one, two = sent(flags, 1, *sides)
            first[pl.ds(row, 1), :] = one
            second[pl.ds(row, 1), :] = two
            row += 1


def spread(flags, block, wide_first, wide_second, narrow_first, narrow_second, corner_first, corner_second, field):
    px, cy, tile = block.shape[1:]
    columns, width = field.shape[1:3]
    rows = rows_of(field)
    empty = jnp.zeros((width, tile), jnp.float32)

    def put(number, pair, values):
        rows[pl.ds((number * columns + HY) * width + pair, cy, stride=width), :] = values

    for number in range(FIELDS):
        for column in range(HY):
            field[number, column] = empty
            field[number, HY + cy + column] = empty
        for pair in range(px):
            put(number, HX + pair, block[number, pair])
        low, high = received(flags, 0, wide_first[number], wide_second[number])
        put(number, HX - 1, low)
        put(number, HX + px, high)
        if number in OUTER_X:
            place = FIELDS + OUTER_X.index(number)
            low, high = received(flags, 0, wide_first[place], wide_second[place])
        else:
            low = high = jnp.zeros((cy, tile), jnp.float32)
        put(number, 0, low)
        put(number, width - 1, high)
    places = [(number, 1 + column, HY + cy + column) for number in range(FIELDS) for column in range(HY - 1)]
    places += [(number, 0, columns - 1) for number in OUTER_Y]
    for place, (number, before, after) in enumerate(places):
        some = pl.ds(place * px, px)
        low, high = received(flags, 1, narrow_first[some, :], narrow_second[some, :])
        field[number, before, pl.ds(HX, px), :] = low
        field[number, after, pl.ds(HX, px), :] = high
    row = 0
    for side in range(2):
        for number, _, pairs, distance in corner_fields():
            pair = HX - pairs if side == 0 else HX + px + pairs - 1
            some = pl.ds(row, 1)
            low, high = received(flags, 1, corner_first[some, :], corner_second[some, :])
            field[number, HY - distance, pl.ds(pair, 1), :] = low
            field[number, HY + cy + distance - 1, pl.ds(pair, 1), :] = high
            row += 1


def lane_half(shape):
    return lax.broadcasted_iota(jnp.int32, shape, len(shape) - 1) < shape[-1] // 2


def swap_half(values):
    return pltpu.roll(values, values.shape[-1] // 2, values.ndim - 1)


def east_of(values, half):
    turned = swap_half(values)
    return jnp.where(half, turned, pltpu.roll(turned, values.shape[-2] - 1, values.ndim - 2))


def west_of(values, half):
    turned = swap_half(values)
    return jnp.where(half, pltpu.roll(turned, 1, values.ndim - 2), turned)


def above(values):
    return pltpu.roll(values, values.shape[-1] - 1, values.ndim - 1)


def below(values):
    return pltpu.roll(values, 1, values.ndim - 1)


def operate(field, coeffs, column, half):
    phases = 3
    here = [field(c, column) for c in range(phases)]
    tx, ty, tz = coeffs[0, column], coeffs[1, column], coeffs[2, column]
    ty_before = coeffs[1, column - 1]
    results = []
    for c in range(phases):
        value = here[c]
        mixed = sum(coeffs[GC + c * phases + b, column] * here[b] for b in range(phases))
        inflow = tx * east_of(value, half) + west_of(tx * value, half)
        inflow = inflow + (ty * field(c, column + 1) + ty_before * field(c, column - 1))
        inflow = inflow + (tz * above(value) + below(tz * value))
        results.append(mixed - inflow)
    return results


def coarse_share(own_misfit, agg_rows, cinv, share, slots, px, cy, narrow):
    count, total = cinv.shape
    lanes = total // share.shape[0]
    width = px + 2 * HX
    agg_no = lax.broadcasted_iota(jnp.int32, (count, own_misfit.shape[-1]), 0)
    parts = [jnp.zeros(agg_no.shape, jnp.float32) for _ in range(4)]
    for column in range(cy):
        for pair in range(px):
            row = column * width + HX + pair
            here = agg_rows[pl.ds(row, 1), :]
            value = own_misfit[pl.ds(row, 1), :]
            spot = (column * px + pair) % len(parts)
            parts[spot] = parts[spot] + jnp.where(agg_no == here, value, 0.0)
    sums = jnp.sum((parts[0] + parts[1]) + (parts[2] + parts[3]), axis=1, keepdims=True)
    wide = share.shape[0]
    for i in range(wide):
        share[pl.ds(i, 1), :] = jnp.sum(cinv[:, i * lanes : (i + 1) * lanes] * sums, axis=0, keepdims=True)
    for i in range(wide):
        for place in range(3):
            row = share[pl.ds((i + place - 1) % wide, 1), :]
            for j in range(narrow):
                slots[i * narrow + j, pl.ds(place, 1), :] = row


def find_misfit(coeffs, current, misfit, own_misfit):
    columns = current.shape[1]
    cy = columns - 2 * HY
    half = lane_half(current.shape[2:])
    for column in range(1, columns - 1):
        applied = operate(lambda c, y: current[c, y], coeffs, column, half)
        for c in range(3):
            value = coeffs[GR + c, column] - applied[c]
            misfit[c, column] = value
            if c == 0 and HY <= column < HY + cy:
                own_misfit[column - HY] = value


def sweep_body(flags, coeffs, current, index, cinv, hot, cold, slots, first, second, third, fourth, px, narrow, scratch, before):
    misfit, work, hold, own_misfit, own_agg, share, update, near_slots, near_corners, sems = scratch
    cy = update.shape[1]
    owned = lax.broadcasted_iota(jnp.int32, current.shape[2:], 0) - HX
    owned = (owned >= 0) & (owned < px)
    before()
    find_misfit(coeffs, current, misfit, own_misfit)
    send = pltpu.make_async_copy(near_slots, slots.at[:, 0], sems.at[0])

    def send_shares():
        for column in range(cy):
            own_agg[column] = index[HY + column] - flags[4]
        coarse_share(rows_of(own_misfit), rows_of(own_agg), cinv, share, near_slots, px, cy, narrow)
        send.start()

    sends = []

    def send_corners():
        near = lane_half(update.shape[2:])
        for number, (x, y) in enumerate(CORNERS):
            rows = []
            for pairs, columns in CORNER_TILES:
                pair = HX + (px - pairs if x > 0 else pairs - 1)
                column = cy - columns if y > 0 else columns - 1
                tile = [update[c, column] for c in range(update.shape[0])]
                if pairs == 2:
                    turned = swap_half(tile[1])
                    tile[0] = jnp.where(near, turned, tile[0]) if x > 0 else jnp.where(near, tile[0], turned)
                    tile = [tile[0], tile[2]]
                rows += [value[pair : pair + 1] for value in tile]
            for spot, row in enumerate(rows):
                near_corners[number, spot // SLOT[1], pl.ds(spot % SLOT[1], 1), :] = row
            target = slots.at[flags[5 + number], pl.ds(1, SLOT[0] - 1)]
            sends.append(pltpu.make_async_copy(near_corners.at[number], target, sems.at[1 + number]))
        for corner in sends:
            corner.start()

    solve(flags, misfit, coeffs, hot, cold, update, first, second, third, fourth, work, hold, send_shares, send_corners)
    for column in range(cy):
        for c in range(update.shape[0]):
            here = jnp.where(owned, update[c, column], 0.0)
            current[c, HY + column] = current[c, HY + column] + here
    send.wait()
    for corner in sends:
        corner.wait()


def prepare(flags, block, wide_first, wide_second, narrow_first, narrow_second, corner_first, corner_second, cinv, hot, cold, coeffs, index, current, slots, first, second, third, fourth, field, *scratch, px, narrow):
    def before():
        got = (wide_first, wide_second, narrow_first, narrow_second, corner_first, corner_second)
        spread(flags, block, *got, field)
        assemble(coeffs, index, current, field)

    sweep_body(flags, coeffs, current, index, cinv, hot, cold, slots, first, second, third, fourth, px, narrow, scratch, before)


def assemble(coeffs, index, current, field):
    columns, width, tile = field.shape[1:]
    half = lane_half((width, tile))
    depth = lax.broadcasted_iota(jnp.int32, (width, tile), 1) % (tile // 2)
    for column in range(columns):
        index[column] = field[IDX, column].astype(jnp.int32)
        for c in range(3):
            current[c, column] = field[CUR + c, column]
    coeffs[1, 0] = field[TY, 0]
    for column in range(1, columns - 1):
        tx, ty = field[TX, column], field[TY, column]
        tz = jnp.where(depth < tile // 2 - 1, field[TZ, column], 0.0)
        faces = (tx + west_of(tx, half)) + (ty + field[TY, column - 1]) + (tz + below(tz))
        coeffs[0, column] = tx
        coeffs[1, column] = ty
        coeffs[2, column] = tz
        for number in range(9):
            value = field[CPL + number, column]
            if number % 4 == 0:
                value = value + faces
                coeffs[GI + number // 4, column] = 1.0 / value
            coeffs[GC + number, column] = value
        for c in range(3):
            coeffs[GR + c, column] = field[RHS + c, column]


def tile_apply(values, coeffs, tiles, columns, first, last):
    stacked = [coeffs[GI + c, column] * value[c] for column, value in zip(columns, values) for c in range(3)]
    width, tile = stacked[0].shape
    stacked = jnp.concatenate(stacked, axis=0)
    pair_no = lax.broadcasted_iota(jnp.int32, stacked.shape, 0) % width
    left = [jnp.where(pair_no == a + HX - 1, stacked, 0.0).astype(jnp.bfloat16) for a in range(first, last)]
    right = tiles[first * tile : last * tile, :]
    result = jnp.dot(jnp.concatenate(left, axis=1), right, preferred_element_type=jnp.float32)
    return [
        [result[(place * 3 + c) * width : (place * 3 + c + 1) * width, place * tile : (place + 1) * tile] for c in range(3)]
        for place in range(2)
    ]


def solve(flags, misfit, coeffs, hot, cold, update, first, second, third, fourth, work, hold, send_shares, send_corners):
    phases, columns = work.shape[:2]
    cy = columns - 2 * HY
    inside = hot.shape[0]
    width, tile = work.shape[2:]
    boxes = hot.shape[1] // tile
    px = width - 2 * HX
    half = lane_half(work.shape[2:])
    side = cold.shape[0] // 2
    groups = 2 * side + inside
    empty = jnp.zeros((width, tile), jnp.float32)

    def tiles(group):
        if group < side:
            return cold.at[group]
        return hot.at[group - side] if group < side + inside else cold.at[group - inside]

    for c in range(phases):
        work[c, 0] = empty
        work[c, columns - 1] = empty

    def pair_of(group):
        return (1 + 2 * group, 2 + 2 * group)

    def start(group):
        values = [[misfit[c, column] for c in range(phases)] for column in pair_of(group)]
        new = tile_apply(values, coeffs, tiles(group), pair_of(group), 0, boxes)
        for column, value in zip(pair_of(group), new):
            for c in range(phases):
                work[c, column] = value[c]

    def step(source, target, shift, group, first_box, last_box):
        needed = [1 < column < columns - 2 for column in pair_of(group)]
        values = []
        for column, want in zip(pair_of(group), needed):
            if want:
                applied = operate(lambda c, y: source[c, y], coeffs, column, half)
                values.append([misfit[c, column] - applied[c] for c in range(phases)])
            else:
                values.append([empty] * phases)
        new = tile_apply(values, coeffs, tiles(group), pair_of(group), first_box, last_box)
        for column, want, value in zip(pair_of(group), needed, new):
            for c in range(phases):
                if want:
                    target[c, column - shift] = source[c, column] + value[c]

    for group in range(groups):
        start(group)
    send_shares()
    for group in range(groups):
        step(work, hold, 0, group, 0, boxes)
    ends = (side, groups - side - 1)
    for group in ends:
        step(hold, update, HY, group, 1, boxes - 1)
    send_corners()
    for group in range(side + 1, groups - side - 1):
        step(hold, update, HY, group, 1, boxes - 1)
    rows = rows_of(update)
    for c in range(phases):
        for pair in range(HX):
            tail = rows[pl.ds(c * cy * width + px + pair, cy, stride=width), :]
            head = rows[pl.ds(c * cy * width + HX + pair, cy, stride=width), :]
            one, two = sent(flags, 0, tail, head)
            first[c, pair] = one
            second[c, pair] = two
        for column in range(HY):
            one, two = sent(flags, 1, update[c, cy - HY + column], update[c, column])
            third[c, column] = one
            fourth[c, column] = two


def advance(flags, current, index, got, slots_in, result):
    phases, columns, width, tile = current.shape
    cy = columns - 2 * HY
    px = width - 2 * HX
    total = [slots_in[d, 0] for d in range(min(4, slots_in.shape[0]))]
    for d in range(4, slots_in.shape[0]):
        total[d % 4] = total[d % 4] + slots_in[d, 0]
    total = sum(total[1:], total[0])
    pair_no = lax.broadcasted_iota(jnp.int32, (width, tile), 0)
    table = jnp.where(pair_no < HX, total[0:1], jnp.where(pair_no < HX + px, total[1:2], total[2:3]))
    owned = (pair_no >= HX) & (pair_no < HX + px)
    near = lane_half((width, tile))
    for column in range(columns):
        for c in range(phases):
            change = 0.0
            if not HY <= column < HY + cy:
                y = -1 if column < HY else 1
                place = column if y < 0 else column - HY - cy
                away = HY - column if y < 0 else place + 1
                change = jnp.where(owned, received(flags, 1, got[2][c, place], got[3][c, place])[(y + 1) // 2], 0.0)
                for number, (x, side) in enumerate(CORNERS):
                    for tile_no, (pairs, distance) in enumerate(CORNER_TILES):
                        if side == y and distance == away:
                            pair = HX - pairs if x < 0 else HX + px + pairs - 1
                            spot = SLOT[1] + 3 * tile_no + (c if pairs == 1 else c // 2)
                            source = slots_in.at[flags[5 + number], spot // SLOT[1], pl.ds(spot % SLOT[1], 1)]
                            row = jnp.broadcast_to(source[...], (width, tile))
                            if pairs == 2:
                                row = swap_half(row) if c == 1 else row
                                row = jnp.where(near, 0.0, row) if x < 0 else jnp.where(near, row, 0.0)
                            change = jnp.where(pair_no == pair, row, change)
            value = current[c, column] + change
            if c == 0:
                value = value + jnp.take_along_axis(table, index[column], axis=1)
            result[c, column] = value
    flat = rows_of(result)
    for c in range(phases):
        for pair in range(HX):
            low, high = received(flags, 0, got[0][c, pair], got[1][c, pair])
            for place, change in ((pair, low), (HX + px + pair, high)):
                where_to = pl.ds((c * columns + HY) * width + place, cy, stride=width)
                flat[where_to, :] = flat[where_to, :] + change


def next_sweep(flags, current, coeffs, index, got_0, got_1, got_2, got_3, slots_in, cinv, hot, cold, result, slots, first, second, third, fourth, *scratch, px, narrow):
    def start():
        advance(flags, current, index, (got_0, got_1, got_2, got_3), slots_in, result)

    sweep_body(flags, coeffs, result, index, cinv, hot, cold, slots, first, second, third, fourth, px, narrow, scratch, start)


def finish(flags, current, coeffs, index, got_0, got_1, got_2, got_3, slots_in, iterate, residual, result, misfit):
    advance(flags, current, index, (got_0, got_1, got_2, got_3), slots_in, result)
    phases, px, cy, _ = iterate.shape
    columns, width = current.shape[1:3]
    half = lane_half(current.shape[2:])
    for column in range(HY, HY + cy):
        applied = operate(lambda c, y: result[c, y], coeffs, column, half)
        for c in range(phases):
            misfit[c, column] = coeffs[GR + c, column] - applied[c]
    for source, target in ((rows_of(result), iterate), (rows_of(misfit), residual)):
        for c in range(phases):
            for pair in range(px):
                target[c, pair] = source[pl.ds((c * columns + HY) * width + HX + pair, cy, stride=width), :]


def swap(first, second, axis):
    count = lax.axis_size(axis)
    if count % 2:
        pairs = [[(i, (i + 1) % count) for i in range(count)], [((i + 1) % count, i) for i in range(count)]]
    else:
        pairs = [
            [(i, i ^ 1) for i in range(count)],
            [(i, (i + 1 if i % 2 else i - 1) % count) for i in range(count)],
        ]
    first = lax.ppermute(first, axis, pairs[0])
    second = lax.ppermute(second, axis, pairs[1])
    return first, second


def order_flags():
    flags = []
    for axis in ("wide", "narrow"):
        place = lax.axis_index(axis) % 2
        odd = lax.axis_size(axis) % 2
        flags += [0, 1] if odd else [place, place]
    flags.append(lax.axis_index("narrow") * AGG_LOC)
    for x, y in CORNERS:
        row = (lax.axis_index("wide") + x) % lax.axis_size("wide")
        flags.append(row * lax.axis_size("narrow") + (lax.axis_index("narrow") + y) % lax.axis_size("narrow"))
    return jnp.stack([jnp.asarray(flag, jnp.int32) for flag in flags])


def per_device(
    rhs,
    start,
    trans,
    accum,
    coupling,
    well_cells,
    well_index,
    agg_map,
    tile_factors,
    coarse_inverse,
):
    phases, px, cy, tile = rhs.shape
    wide, narrow = lax.axis_size("wide"), lax.axis_size("narrow")
    width, columns = px + 2 * HX, cy + 2 * HY
    f32 = jnp.float32
    flags = order_flags()
    lanes = narrow * AGG_LOC
    if min(wide, narrow) < 3 or lanes != tile:
        raise ValueError("unsupported mesh")

    boxes, count = tile_factors.shape[:2]
    if HY != 3 or COLD != 2 or cy % 2:
        raise ValueError("unsupported sizes")
    cold = ((COLD, boxes * tile, 2 * tile), tile_factors.dtype)
    hot = ((count // 2 - COLD, boxes * tile, 2 * tile), tile_factors.dtype)

    face = ((FIELDS + len(OUTER_X), cy, tile), f32)
    block, first, second = call(
        pack_wide,
        [((FIELDS, px, cy, tile), f32), face, face],
        [
            pltpu.VMEM((px, cy, tile), jnp.int32),
            pltpu.VMEM((px, cy, tile), f32),
            pltpu.VMEM(well_cells.shape, jnp.int32),
            pltpu.VMEM(well_index.shape, f32),
            pltpu.SemaphoreType.DMA((7 + phases,)),
        ],
        far=range(8),
    )(flags, trans, accum, coupling, rhs, start, agg_map, well_cells, well_index)
    got = swap(first, second, "wide")
    face = ((narrow_rows(px), tile), f32)
    got += swap(*call(pack_narrow, [face, face])(flags, block), "narrow")
    cold_tiles, hot_tiles, kept = call(
        turn,
        [cold, hot, cold],
        [pltpu.VMEM(tile_factors.shape, tile_factors.dtype), pltpu.SemaphoreType.DMA((count // 2 + 1,))],
        far=(0,),
        far_outs=(2,),
    )(flags, tile_factors, block)
    face = ((CORNER_ROWS, tile), f32)
    got += swap(*call(pack_corners, [face, face])(flags, *got[:2]), "narrow")

    vec = (width, tile)
    field = ((phases, columns) + vec, f32)
    inner = ((phases, columns - 1) + vec, f32)
    slot = ((wide * narrow,) + SLOT + (lanes,), f32)
    part = ((phases, cy) + vec, f32)
    face = ((phases, HX, cy, tile), f32)
    edge_face = ((phases, HY) + vec, f32)
    scratch = [
        pltpu.VMEM(*inner),
        pltpu.VMEM(*field),
        pltpu.VMEM(*field),
        pltpu.VMEM((cy,) + vec, f32),
        pltpu.VMEM((cy,) + vec, jnp.int32),
        pltpu.VMEM((wide, lanes), f32),
        pltpu.VMEM(*part),
        pltpu.VMEM((wide * narrow,) + SLOT[1:] + (lanes,), f32),
        pltpu.VMEM((len(CORNERS), SLOT[0] - 1) + SLOT[1:] + (lanes,), f32),
        pltpu.SemaphoreType.DMA((1 + len(CORNERS),)),
    ]
    faces = [face, face, edge_face, edge_face]
    coeffs, index, current, slots, *sends = call(
        functools.partial(prepare, px=px, narrow=narrow),
        [((GFIELDS, columns - 1) + vec, f32), ((columns,) + vec, jnp.int32), field, slot] + faces,
        [pltpu.VMEM((FIELDS, columns) + vec, f32)] + scratch,
        far_outs=(3,),
    )(flags, block, *got, coarse_inverse, hot_tiles, cold_tiles)
    for sweep in range(SWEEPS):
        gathered = lax.all_to_all(slots, ("wide", "narrow"), 0, 0, tiled=True)
        got = swap(*sends[:2], "wide") + swap(*sends[2:], "narrow")
        if sweep < SWEEPS - 1:
            (cold_tiles,) = call(fetch, [cold], [pltpu.SemaphoreType.DMA((COLD,))], far=(0,))(flags, kept, gathered)
        if sweep < SWEEPS - 1:
            current, slots, *sends = call(
                functools.partial(next_sweep, px=px, narrow=narrow),
                [field, slot] + faces,
                scratch,
                far_outs=(1,),
            )(flags, current, coeffs, index, *got, gathered, coarse_inverse, hot_tiles, cold_tiles)
    out = (rhs.shape, f32)
    return call(finish, [out, out], [pltpu.VMEM(*field), pltpu.VMEM(*field)])(
        flags, current, coeffs, index, *got, gathered
    )


def solution(mesh):
    return jax.shard_map(
        per_device,
        mesh=mesh,
        in_specs=(
            P(None, "wide", "narrow", None),
            P(None, "wide", "narrow", None),
            P(None, "wide", "narrow", None),
            P("wide", "narrow", None),
            P(None, None, "wide", "narrow", None),
            P("wide", "narrow", None),
            P("wide", "narrow", None),
            P("wide", "narrow", None),
            P("wide", "narrow", None, None),
            P(("wide", "narrow"), None),
        ),
        out_specs=(P(None, "wide", "narrow", None), P(None, "wide", "narrow", None)),
        check_vma=False,
    )
```

```python
import functools

import jax
import jax.numpy as jnp
from jax import lax
from jax.experimental import pallas as pl
from jax.experimental.pallas import tpu as pltpu
from jax.sharding import PartitionSpec as P

AGG_LOC = 32
SWEEPS = 3
HX = 2
HY = 3

TX, TY, TZ, CPL, RHS, CUR, IDX, FIELDS = 0, 1, 2, 3, 12, 15, 18, 19
OUTER_X = (TX, CUR, CUR + 1, CUR + 2, IDX)
OUTER_Y = (TY, CUR, CUR + 1, CUR + 2, IDX)
NEXT_Y = (TX,) + OUTER_Y
NEXT_X = OUTER_X
CORNERS = ((-1, -1), (-1, 1), (1, -1), (1, 1))
CORNER_TILES = ((1, 1), (1, 2), (2, 1))
COLD = 2
SLOT = (3, 4)
GC, GI, GR, GFIELDS = 3, 12, 15, 18

PARAMS = pltpu.CompilerParams(vmem_limit_bytes=16 * 1024 * 1024)


HBM = pl.BlockSpec(memory_space=pltpu.HBM)
VMEM = pl.BlockSpec(memory_space=pltpu.VMEM)


def call(body, outs, scratch=(), far=(), far_outs=()):
    def run(flags, *args):
        specs = [pl.BlockSpec(memory_space=pltpu.SMEM)]
        specs += [HBM if number in far else VMEM for number in range(len(args))]
        args = [
            pltpu.with_memory_space_constraint(arg, pltpu.HBM) if number in far else arg
            for number, arg in enumerate(args)
        ]
        return pl.pallas_call(
            body,
            out_shape=tuple(
                (pltpu.HBM if number in far_outs else jax.ShapeDtypeStruct)(*out) for number, out in enumerate(outs)
            ),
            in_specs=specs,
            out_specs=tuple(HBM if number in far_outs else VMEM for number in range(len(outs))),
            scratch_shapes=list(scratch),
            compiler_params=PARAMS,
        )(flags, *args)

    return run


def rows_of(ref):
    size = 1
    for length in ref.shape[:-1]:
        size *= length
    return ref.reshape(size, ref.shape[-1])


def sent(flags, axis, tail, head):
    low_first = flags[2 * axis] == 0
    return jnp.where(low_first, tail, head), jnp.where(low_first, head, tail)


def received(flags, axis, first, second):
    swapped = flags[2 * axis + 1] == 0
    return jnp.where(swapped, second, first), jnp.where(swapped, first, second)


def split3(values):
    high = values.astype(jnp.bfloat16)
    rest = values - high.astype(jnp.float32)
    middle = rest.astype(jnp.bfloat16)
    low = (rest - middle.astype(jnp.float32)).astype(jnp.bfloat16)
    return high, middle, low


def nt_dot(left, right):
    return lax.dot_general(left, right, (((1,), (1,)), ((), ())), preferred_element_type=jnp.float32)


def turn(flags, factors, after, cold, hot, kept, raw, sems):
    boxes, count, tile, _ = factors.shape
    side = cold.shape[0] // 2
    inside = hot.shape[0]
    order = sorted(range(count // 2), key=lambda group: side <= group < side + inside)
    loads = {}
    for group in order:
        some = pl.ds(2 * group, 2)
        loads[group] = pltpu.make_async_copy(factors.at[:, some], raw.at[:, some], sems.at[group])
        loads[group].start()
    save = pltpu.make_async_copy(cold, kept, sems.at[count // 2])
    row_no = lax.broadcasted_iota(jnp.int32, (tile, tile), 0)
    unit = jnp.where(row_no == lax.broadcasted_iota(jnp.int32, (tile, tile), 1), 1.0, 0.0).astype(factors.dtype)
    for number, group in enumerate(order):
        if number == 2 * side:
            save.start()
        loads[group].wait()
        if group < side:
            target = cold.at[group]
        elif group < side + inside:
            target = hot.at[group - side]
        else:
            target = cold.at[group - inside]
        for place in range(2):
            stacked = jnp.concatenate([raw[a, 2 * group + place] for a in range(boxes)], axis=0)
            turned = nt_dot(unit, stacked).astype(factors.dtype)
            for a in range(boxes):
                spot = (pl.ds(a * tile, tile), pl.ds(place * tile, tile))
                target[spot] = turned[:, a * tile : (a + 1) * tile]
    save.wait()


def fetch(flags, kept, after, cold, sems):
    rows = cold.shape[1] // (sems.shape[0] // cold.shape[0])
    loads = []
    for number in range(sems.shape[0]):
        spot = (number % cold.shape[0], pl.ds(number // cold.shape[0] * rows, rows))
        loads.append(pltpu.make_async_copy(kept.at[spot], cold.at[spot], sems.at[number]))
    for load in loads:
        load.start()
    for load in loads:
        load.wait()


def pack_wide(flags, trans, accum, coupling, rhs, start, agg, far_cells, far_index, block, first, second, groups, near_accum, cells, index, sems):
    phases, px, cy, tile = rhs.shape
    conn = cells.shape[-1]
    copies = [
        (far_cells, cells),
        (far_index, index),
        (accum, near_accum),
        (agg, groups),
        (trans, block.at[pl.ds(TX, 3)]),
        (rhs, block.at[pl.ds(RHS, phases)]),
        (start, block.at[pl.ds(CUR, phases)]),
    ]
    copies += [(coupling.at[c], block.at[pl.ds(CPL + c * phases, phases)]) for c in range(phases)]
    copies = [pltpu.make_async_copy(source, target, sems.at[k]) for k, (source, target) in enumerate(copies)]
    for copy in copies:
        copy.start()
    for copy in copies[:2]:
        copy.wait()
    where_to = cells[0]
    row_no = lax.broadcasted_iota(jnp.int32, (px * cy, conn), 0)
    lane_no = lax.broadcasted_iota(jnp.int32, (tile, conn), 0)
    lanes = jnp.where(lane_no == where_to % tile, 1.0, 0.0).astype(jnp.bfloat16)
    rows = jnp.where(row_no == where_to // tile, index[0], 0.0)
    added = sum(nt_dot(part, lanes) for part in split3(rows))
    for copy in copies[2:]:
        copy.wait()
    for pair in range(px):
        accum_w = near_accum[pair] + added[pair * cy : (pair + 1) * cy]
        for c in range(phases):
            number = CPL + c * phases + c
            block[number, pair] = block[number, pair] + accum_w
        block[IDX, pair] = (groups[pair] + flags[4]).astype(jnp.float32)
    for number in range(FIELDS):
        one, two = sent(flags, 0, block[number, px - 1], block[number, 0])
        first[number] = one
        second[number] = two
    for place, number in enumerate(OUTER_X):
        one, two = sent(flags, 0, block[number, px - 2], block[number, 1])
        first[FIELDS + place] = one
        second[FIELDS + place] = two


def narrow_rows(px):
    return -(-(FIELDS * (HY - 1) + len(OUTER_Y)) * px // 8) * 8


CORNER_ROWS = -(-2 * (FIELDS + len(NEXT_Y) + len(NEXT_X)) // 8) * 8


def pack_narrow(flags, block, first, second):
    px, cy, _ = block.shape[1:]
    rows = rows_of(block)

    def put(place, number, tail, head):
        sides = [rows[pl.ds(number * px * cy + column, px, stride=cy), :] for column in (tail, head)]
        one, two = sent(flags, 1, *sides)
        first[pl.ds(place * px, px), :] = one
        second[pl.ds(place * px, px), :] = two

    for number in range(FIELDS):
        for column in range(HY - 1):
            put(number * (HY - 1) + column, number, cy - HY + 1 + column, column)
    for place, number in enumerate(OUTER_Y):
        put(FIELDS * (HY - 1) + place, number, cy - HY, HY - 1)


def corner_fields():
    rows = [(number, number, 1, 1) for number in range(FIELDS)]
    rows += [(number, number, 1, 2) for number in NEXT_Y]
    return rows + [(number, FIELDS + place, 2, 1) for place, number in enumerate(NEXT_X)]


def pack_corners(flags, got_first, got_second, first, second):
    cy = got_first.shape[1]
    row = 0
    for side in range(2):
        for _, place, _, distance in corner_fields():
            sides = []
            for column in (cy - distance, distance - 1):
                pair = [got[place, pl.ds(column, 1), :] for got in (got_first, got_second)]
                sides.append(received(flags, 0, *pair)[side])
            one, two = sent(flags, 1, *sides)
            first[pl.ds(row, 1), :] = one
            second[pl.ds(row, 1), :] = two
            row += 1


def spread(flags, block, wide_first, wide_second, narrow_first, narrow_second, corner_first, corner_second, field):
    px, cy, tile = block.shape[1:]
    columns, width = field.shape[1:3]
    rows = rows_of(field)
    empty = jnp.zeros((width, tile), jnp.float32)

    def put(number, pair, values):
        rows[pl.ds((number * columns + HY) * width + pair, cy, stride=width), :] = values

    for number in range(FIELDS):
        for column in range(HY):
            field[number, column] = empty
            field[number, HY + cy + column] = empty
        for pair in range(px):
            put(number, HX + pair, block[number, pair])
        low, high = received(flags, 0, wide_first[number], wide_second[number])
        put(number, HX - 1, low)
        put(number, HX + px, high)
        if number in OUTER_X:
            place = FIELDS + OUTER_X.index(number)
            low, high = received(flags, 0, wide_first[place], wide_second[place])
        else:
            low = high = jnp.zeros((cy, tile), jnp.float32)
        put(number, 0, low)
        put(number, width - 1, high)
    places = [(number, 1 + column, HY + cy + column) for number in range(FIELDS) for column in range(HY - 1)]
    places += [(number, 0, columns - 1) for number in OUTER_Y]
    for place, (number, before, after) in enumerate(places):
        some = pl.ds(place * px, px)
        low, high = received(flags, 1, narrow_first[some, :], narrow_second[some, :])
        field[number, before, pl.ds(HX, px), :] = low
        field[number, after, pl.ds(HX, px), :] = high
    row = 0
    for side in range(2):
        for number, _, pairs, distance in corner_fields():
            pair = HX - pairs if side == 0 else HX + px + pairs - 1
            some = pl.ds(row, 1)
            low, high = received(flags, 1, corner_first[some, :], corner_second[some, :])
            field[number, HY - distance, pl.ds(pair, 1), :] = low
            field[number, HY + cy + distance - 1, pl.ds(pair, 1), :] = high
            row += 1


def lane_half(shape):
    return lax.broadcasted_iota(jnp.int32, shape, len(shape) - 1) < shape[-1] // 2


def swap_half(values):
    return pltpu.roll(values, values.shape[-1] // 2, values.ndim - 1)


def east_of(values, half):
    turned = swap_half(values)
    return jnp.where(half, turned, pltpu.roll(turned, values.shape[-2] - 1, values.ndim - 2))


def west_of(values, half):
    turned = swap_half(values)
    return jnp.where(half, pltpu.roll(turned, 1, values.ndim - 2), turned)


def above(values):
    return pltpu.roll(values, values.shape[-1] - 1, values.ndim - 1)


def below(values):
    return pltpu.roll(values, 1, values.ndim - 1)


def operate(field, coeffs, column, half):
    phases = 3
    here = [field(c, column) for c in range(phases)]
    tx, ty, tz = coeffs[0, column], coeffs[1, column], coeffs[2, column]
    ty_before = coeffs[1, column - 1]
    results = []
    for c in range(phases):
        value = here[c]
        mixed = sum(coeffs[GC + c * phases + b, column] * here[b] for b in range(phases))
        inflow = tx * east_of(value, half) + west_of(tx * value, half)
        inflow = inflow + (ty * field(c, column + 1) + ty_before * field(c, column - 1))
        inflow = inflow + (tz * above(value) + below(tz * value))
        results.append(mixed - inflow)
    return results


def coarse_share(own_misfit, agg_rows, cinv, share, slots, px, cy, narrow):
    count, total = cinv.shape
    lanes = total // share.shape[0]
    width = px + 2 * HX
    agg_no = lax.broadcasted_iota(jnp.int32, (count, own_misfit.shape[-1]), 0)
    parts = [jnp.zeros(agg_no.shape, jnp.float32) for _ in range(4)]
    for column in range(cy):
        for pair in range(px):
            row = column * width + HX + pair
            here = agg_rows[pl.ds(row, 1), :]
            value = own_misfit[pl.ds(row, 1), :]
            spot = (column * px + pair) % len(parts)
            parts[spot] = parts[spot] + jnp.where(agg_no == here, value, 0.0)
    sums = jnp.sum((parts[0] + parts[1]) + (parts[2] + parts[3]), axis=1, keepdims=True)
    wide = share.shape[0]
    for i in range(wide):
        share[pl.ds(i, 1), :] = jnp.sum(cinv[:, i * lanes : (i + 1) * lanes] * sums, axis=0, keepdims=True)
    for i in range(wide):
        for place in range(3):
            row = share[pl.ds((i + place - 1) % wide, 1), :]
            for j in range(narrow):
                slots[i * narrow + j, pl.ds(place, 1), :] = row


def find_misfit(coeffs, current, misfit, own_misfit):
    columns = current.shape[1]
    cy = columns - 2 * HY
    half = lane_half(current.shape[2:])
    for column in range(1, columns - 1):
        applied = operate(lambda c, y: current[c, y], coeffs, column, half)
        for c in range(3):
            value = coeffs[GR + c, column] - applied[c]
            misfit[c, column] = value
            if c == 0 and HY <= column < HY + cy:
                own_misfit[column - HY] = value


def sweep_body(flags, coeffs, current, index, cinv, hot, cold, slots, first, second, third, fourth, px, narrow, scratch, before):
    misfit, work, hold, own_misfit, own_agg, share, update, near_slots, near_corners, sems = scratch
    cy = update.shape[1]
    owned = lax.broadcasted_iota(jnp.int32, current.shape[2:], 0) - HX
    owned = (owned >= 0) & (owned < px)
    before()
    find_misfit(coeffs, current, misfit, own_misfit)
    send = pltpu.make_async_copy(near_slots, slots.at[:, 0], sems.at[0])

    def send_shares():
        for column in range(cy):
            own_agg[column] = index[HY + column] - flags[4]
        coarse_share(rows_of(own_misfit), rows_of(own_agg), cinv, share, near_slots, px, cy, narrow)
        send.start()

    sends = []

    def send_corners():
        if slots.shape[1] == 1:
            return
        near = lane_half(update.shape[2:])
        for number, (x, y) in enumerate(CORNERS):
            rows = []
            for pairs, columns in CORNER_TILES:
                pair = HX + (px - pairs if x > 0 else pairs - 1)
                column = cy - columns if y > 0 else columns - 1
                tile = [update[c, column] for c in range(update.shape[0])]
                if pairs == 2:
                    turned = swap_half(tile[1])
                    tile[0] = jnp.where(near, turned, tile[0]) if x > 0 else jnp.where(near, tile[0], turned)
                    tile = [tile[0], tile[2]]
                rows += [value[pair : pair + 1] for value in tile]
            for spot, row in enumerate(rows):
                near_corners[number, spot // SLOT[1], pl.ds(spot % SLOT[1], 1), :] = row
            target = slots.at[flags[5 + number], pl.ds(1, SLOT[0] - 1)]
            sends.append(pltpu.make_async_copy(near_corners.at[number], target, sems.at[1 + number]))
        for corner in sends:
            corner.start()

    solve(flags, misfit, coeffs, hot, cold, update, first, second, third, fourth, work, hold, send_shares, send_corners)
    for column in range(cy):
        for c in range(update.shape[0]):
            here = jnp.where(owned, update[c, column], 0.0)
            current[c, HY + column] = current[c, HY + column] + here
    send.wait()
    for corner in sends:
        corner.wait()


def prepare(flags, block, wide_first, wide_second, narrow_first, narrow_second, corner_first, corner_second, cinv, hot, cold, coeffs, index, current, slots, first, second, third, fourth, field, *scratch, px, narrow):
    def before():
        got = (wide_first, wide_second, narrow_first, narrow_second, corner_first, corner_second)
        spread(flags, block, *got, field)
        assemble(coeffs, index, current, field)

    sweep_body(flags, coeffs, current, index, cinv, hot, cold, slots, first, second, third, fourth, px, narrow, scratch, before)


def assemble(coeffs, index, current, field):
    columns, width, tile = field.shape[1:]
    half = lane_half((width, tile))
    depth = lax.broadcasted_iota(jnp.int32, (width, tile), 1) % (tile // 2)
    for column in range(columns):
        index[column] = field[IDX, column].astype(jnp.int32)
        for c in range(3):
            current[c, column] = field[CUR + c, column]
    coeffs[1, 0] = field[TY, 0]
    for column in range(1, columns - 1):
        tx, ty = field[TX, column], field[TY, column]
        tz = jnp.where(depth < tile // 2 - 1, field[TZ, column], 0.0)
        faces = (tx + west_of(tx, half)) + (ty + field[TY, column - 1]) + (tz + below(tz))
        coeffs[0, column] = tx
        coeffs[1, column] = ty
        coeffs[2, column] = tz
        for number in range(9):
            value = field[CPL + number, column]
            if number % 4 == 0:
                value = value + faces
                coeffs[GI + number // 4, column] = 1.0 / value
            coeffs[GC + number, column] = value
        for c in range(3):
            coeffs[GR + c, column] = field[RHS + c, column]


def tile_apply(values, coeffs, tiles, columns, first, last):
    stacked = [coeffs[GI + c, column] * value[c] for column, value in zip(columns, values) for c in range(3)]
    width, tile = stacked[0].shape
    stacked = jnp.concatenate(stacked, axis=0)
    pair_no = lax.broadcasted_iota(jnp.int32, stacked.shape, 0) % width
    left = [jnp.where(pair_no == a + HX - 1, stacked, 0.0).astype(jnp.bfloat16) for a in range(first, last)]
    right = tiles[first * tile : last * tile, :]
    result = jnp.dot(jnp.concatenate(left, axis=1), right, preferred_element_type=jnp.float32)
    return [
        [result[(place * 3 + c) * width : (place * 3 + c + 1) * width, place * tile : (place + 1) * tile] for c in range(3)]
        for place in range(2)
    ]


def solve(flags, misfit, coeffs, hot, cold, update, first, second, third, fourth, work, hold, send_shares, send_corners):
    phases, columns = work.shape[:2]
    cy = columns - 2 * HY
    inside = hot.shape[0]
    width, tile = work.shape[2:]
    boxes = hot.shape[1] // tile
    px = width - 2 * HX
    half = lane_half(work.shape[2:])
    side = cold.shape[0] // 2
    groups = 2 * side + inside
    empty = jnp.zeros((width, tile), jnp.float32)

    def tiles(group):
        if group < side:
            return cold.at[group]
        return hot.at[group - side] if group < side + inside else cold.at[group - inside]

    for c in range(phases):
        work[c, 0] = empty
        work[c, columns - 1] = empty

    def pair_of(group):
        return (1 + 2 * group, 2 + 2 * group)

    def start(group):
        values = [[misfit[c, column] for c in range(phases)] for column in pair_of(group)]
        new = tile_apply(values, coeffs, tiles(group), pair_of(group), 0, boxes)
        for column, value in zip(pair_of(group), new):
            for c in range(phases):
                work[c, column] = value[c]

    def step(source, target, shift, group, first_box, last_box):
        needed = [1 < column < columns - 2 for column in pair_of(group)]
        values = []
        for column, want in zip(pair_of(group), needed):
            if want:
                applied = operate(lambda c, y: source[c, y], coeffs, column, half)
                values.append([misfit[c, column] - applied[c] for c in range(phases)])
            else:
                values.append([empty] * phases)
        new = tile_apply(values, coeffs, tiles(group), pair_of(group), first_box, last_box)
        for column, want, value in zip(pair_of(group), needed, new):
            for c in range(phases):
                if want:
                    target[c, column - shift] = source[c, column] + value[c]

    for group in range(groups):
        start(group)
    send_shares()
    for group in range(groups):
        step(work, hold, 0, group, 0, boxes)
    ends = (side, groups - side - 1)
    for group in ends:
        step(hold, update, HY, group, 1, boxes - 1)
    send_corners()
    for group in range(side + 1, groups - side - 1):
        step(hold, update, HY, group, 1, boxes - 1)
    rows = rows_of(update)
    for c in range(phases):
        for pair in range(HX):
            tail = rows[pl.ds(c * cy * width + px + pair, cy, stride=width), :]
            head = rows[pl.ds(c * cy * width + HX + pair, cy, stride=width), :]
            one, two = sent(flags, 0, tail, head)
            first[c, pair] = one
            second[c, pair] = two
        for column in range(HY):
            one, two = sent(flags, 1, update[c, cy - HY + column], update[c, column])
            third[c, column] = one
            fourth[c, column] = two


def advance(flags, current, index, got, slots_in, result):
    phases, columns, width, tile = current.shape
    cy = columns - 2 * HY
    px = width - 2 * HX
    total = [slots_in[d, 0] for d in range(min(4, slots_in.shape[0]))]
    for d in range(4, slots_in.shape[0]):
        total[d % 4] = total[d % 4] + slots_in[d, 0]
    total = sum(total[1:], total[0])
    pair_no = lax.broadcasted_iota(jnp.int32, (width, tile), 0)
    table = jnp.where(pair_no < HX, total[0:1], jnp.where(pair_no < HX + px, total[1:2], total[2:3]))
    owned = (pair_no >= HX) & (pair_no < HX + px)
    near = lane_half((width, tile))
    for column in range(columns):
        for c in range(phases):
            change = 0.0
            if not HY <= column < HY + cy:
                y = -1 if column < HY else 1
                place = column if y < 0 else column - HY - cy
                away = HY - column if y < 0 else place + 1
                change = jnp.where(owned, received(flags, 1, got[2][c, place], got[3][c, place])[(y + 1) // 2], 0.0)
                for number, (x, side) in enumerate(CORNERS if slots_in.shape[1] > 1 else ()):
                    for tile_no, (pairs, distance) in enumerate(CORNER_TILES):
                        if side == y and distance == away:
                            pair = HX - pairs if x < 0 else HX + px + pairs - 1
                            spot = SLOT[1] + 3 * tile_no + (c if pairs == 1 else c // 2)
                            source = slots_in.at[flags[5 + number], spot // SLOT[1], pl.ds(spot % SLOT[1], 1)]
                            row = jnp.broadcast_to(source[...], (width, tile))
                            if pairs == 2:
                                row = swap_half(row) if c == 1 else row
                                row = jnp.where(near, 0.0, row) if x < 0 else jnp.where(near, row, 0.0)
                            change = jnp.where(pair_no == pair, row, change)
            value = current[c, column] + change
            if c == 0:
                value = value + jnp.take_along_axis(table, index[column], axis=1)
            result[c, column] = value
    flat = rows_of(result)
    for c in range(phases):
        for pair in range(HX):
            low, high = received(flags, 0, got[0][c, pair], got[1][c, pair])
            for place, change in ((pair, low), (HX + px + pair, high)):
                where_to = pl.ds((c * columns + HY) * width + place, cy, stride=width)
                flat[where_to, :] = flat[where_to, :] + change


def next_sweep(flags, current, coeffs, index, got_0, got_1, got_2, got_3, slots_in, cinv, hot, cold, result, slots, first, second, third, fourth, *scratch, px, narrow):
    def start():
        advance(flags, current, index, (got_0, got_1, got_2, got_3), slots_in, result)

    sweep_body(flags, coeffs, result, index, cinv, hot, cold, slots, first, second, third, fourth, px, narrow, scratch, start)


def finish(flags, current, coeffs, index, got_0, got_1, got_2, got_3, slots_in, iterate, residual, result, misfit):
    advance(flags, current, index, (got_0, got_1, got_2, got_3), slots_in, result)
    phases, px, cy, _ = iterate.shape
    columns, width = current.shape[1:3]
    half = lane_half(current.shape[2:])
    for column in range(HY, HY + cy):
        applied = operate(lambda c, y: result[c, y], coeffs, column, half)
        for c in range(phases):
            misfit[c, column] = coeffs[GR + c, column] - applied[c]
    for source, target in ((rows_of(result), iterate), (rows_of(misfit), residual)):
        for c in range(phases):
            for pair in range(px):
                target[c, pair] = source[pl.ds((c * columns + HY) * width + HX + pair, cy, stride=width), :]


def swap(first, second, axis):
    count = lax.axis_size(axis)
    if count % 2:
        pairs = [[(i, (i + 1) % count) for i in range(count)], [((i + 1) % count, i) for i in range(count)]]
    else:
        pairs = [
            [(i, i ^ 1) for i in range(count)],
            [(i, (i + 1 if i % 2 else i - 1) % count) for i in range(count)],
        ]
    first = lax.ppermute(first, axis, pairs[0])
    second = lax.ppermute(second, axis, pairs[1])
    return first, second


def order_flags():
    flags = []
    for axis in ("wide", "narrow"):
        place = lax.axis_index(axis) % 2
        odd = lax.axis_size(axis) % 2
        flags += [0, 1] if odd else [place, place]
    flags.append(lax.axis_index("narrow") * AGG_LOC)
    for x, y in CORNERS:
        row = (lax.axis_index("wide") + x) % lax.axis_size("wide")
        flags.append(row * lax.axis_size("narrow") + (lax.axis_index("narrow") + y) % lax.axis_size("narrow"))
    return jnp.stack([jnp.asarray(flag, jnp.int32) for flag in flags])


def per_device(
    rhs,
    start,
    trans,
    accum,
    coupling,
    well_cells,
    well_index,
    agg_map,
    tile_factors,
    coarse_inverse,
):
    phases, px, cy, tile = rhs.shape
    wide, narrow = lax.axis_size("wide"), lax.axis_size("narrow")
    width, columns = px + 2 * HX, cy + 2 * HY
    f32 = jnp.float32
    flags = order_flags()
    lanes = narrow * AGG_LOC
    if min(wide, narrow) < 3 or lanes != tile:
        raise ValueError("unsupported mesh")

    boxes, count = tile_factors.shape[:2]
    if HY != 3 or COLD != 2 or cy % 2:
        raise ValueError("unsupported sizes")
    cold = ((COLD, boxes * tile, 2 * tile), tile_factors.dtype)
    hot = ((count // 2 - COLD, boxes * tile, 2 * tile), tile_factors.dtype)

    face = ((FIELDS + len(OUTER_X), cy, tile), f32)
    block, first, second = call(
        pack_wide,
        [((FIELDS, px, cy, tile), f32), face, face],
        [
            pltpu.VMEM((px, cy, tile), jnp.int32),
            pltpu.VMEM((px, cy, tile), f32),
            pltpu.VMEM(well_cells.shape, jnp.int32),
            pltpu.VMEM(well_index.shape, f32),
            pltpu.SemaphoreType.DMA((7 + phases,)),
        ],
        far=range(8),
    )(flags, trans, accum, coupling, rhs, start, agg_map, well_cells, well_index)
    got = swap(first, second, "wide")
    face = ((narrow_rows(px), tile), f32)
    got += swap(*call(pack_narrow, [face, face])(flags, block), "narrow")
    cold_tiles, hot_tiles, kept = call(
        turn,
        [cold, hot, cold],
        [pltpu.VMEM(tile_factors.shape, tile_factors.dtype), pltpu.SemaphoreType.DMA((count // 2 + 1,))],
        far=(0,),
        far_outs=(2,),
    )(flags, tile_factors, block)
    face = ((CORNER_ROWS, tile), f32)
    got += swap(*call(pack_corners, [face, face])(flags, *got[:2]), "narrow")

    vec = (width, tile)
    field = ((phases, columns) + vec, f32)
    inner = ((phases, columns - 1) + vec, f32)
    slot = ((wide * narrow,) + SLOT + (lanes,), f32)
    last_slot = ((wide * narrow, 1) + SLOT[1:] + (lanes,), f32)
    part = ((phases, cy) + vec, f32)
    face = ((phases, HX, cy, tile), f32)
    edge_face = ((phases, HY) + vec, f32)
    scratch = [
        pltpu.VMEM(*inner),
        pltpu.VMEM(*field),
        pltpu.VMEM(*field),
        pltpu.VMEM((cy,) + vec, f32),
        pltpu.VMEM((cy,) + vec, jnp.int32),
        pltpu.VMEM((wide, lanes), f32),
        pltpu.VMEM(*part),
        pltpu.VMEM((wide * narrow,) + SLOT[1:] + (lanes,), f32),
        pltpu.VMEM((len(CORNERS), SLOT[0] - 1) + SLOT[1:] + (lanes,), f32),
        pltpu.SemaphoreType.DMA((1 + len(CORNERS),)),
    ]
    faces = [face, face, edge_face, edge_face]
    coeffs, index, current, slots, *sends = call(
        functools.partial(prepare, px=px, narrow=narrow),
        [((GFIELDS, columns - 1) + vec, f32), ((columns,) + vec, jnp.int32), field, slot] + faces,
        [pltpu.VMEM((FIELDS, columns) + vec, f32)] + scratch,
        far_outs=(3,),
    )(flags, block, *got, coarse_inverse, hot_tiles, cold_tiles)
    for sweep in range(SWEEPS):
        gathered = lax.all_to_all(slots, ("wide", "narrow"), 0, 0, tiled=True)
        got = swap(*sends[:2], "wide") + swap(*sends[2:], "narrow")
        if sweep < SWEEPS - 1:
            (cold_tiles,) = call(fetch, [cold], [pltpu.SemaphoreType.DMA((COLD,))], far=(0,))(flags, kept, gathered)
        if sweep < SWEEPS - 1:
            current, slots, *sends = call(
                functools.partial(next_sweep, px=px, narrow=narrow),
                [field, slot if sweep < SWEEPS - 2 else last_slot] + faces,
                scratch,
                far_outs=(1,),
            )(flags, current, coeffs, index, *got, gathered, coarse_inverse, hot_tiles, cold_tiles)
    out = (rhs.shape, f32)
    return call(finish, [out, out], [pltpu.VMEM(*field), pltpu.VMEM(*field)])(
        flags, current, coeffs, index, *got, gathered
    )


def solution(mesh):
    return jax.shard_map(
        per_device,
        mesh=mesh,
        in_specs=(
            P(None, "wide", "narrow", None),
            P(None, "wide", "narrow", None),
            P(None, "wide", "narrow", None),
            P("wide", "narrow", None),
            P(None, None, "wide", "narrow", None),
            P("wide", "narrow", None),
            P("wide", "narrow", None),
            P("wide", "narrow", None),
            P("wide", "narrow", None, None),
            P(("wide", "narrow"), None),
        ),
        out_specs=(P(None, "wide", "narrow", None), P(None, "wide", "narrow", None)),
        check_vma=False,
    )
```
